32 devices in a mesh: row: 8 (over z, y), ta: 4 (over x, core).
Axes of the slice: x: 2, y: 2, z: 4, core: 2. Of those that a mesh axis runs over, the one named last changes fastest.
Arguments:
- hidden: bfloat16 [8, 256, 3584], P('row', None, 'ta'), may hold values from -6 to 6
- target: bfloat16 [8, 256, 3584], P('row', None, 'ta'), may hold values from -6 to 6
- w_down: bfloat16 [8, 2, 3584, 256], P('row', None, 'ta'), may hold values from -5 to 5
- w_up: bfloat16 [8, 2, 256, 3584], P('row', None, None, 'ta'), may hold values from -5 to 5
- m_down: float32 [8, 2, 3584, 256], P('row', None, 'ta'), may hold values from -9 to 9
- m_up: float32 [8, 2, 256, 3584], P('row', None, None, 'ta'), may hold values from -9 to 9
Outputs:
- avg_down: bfloat16 [2, 3584, 256], P(None, 'ta')
- avg_up: bfloat16 [2, 256, 3584], P(None, None, 'ta')
- mom_down: float32 [2, 3584, 256], P(None, 'ta')
- mom_up: float32 [2, 256, 3584], P(None, None, 'ta')
The draws below stay inside these ranges and needn't reach their ends.
All inputs are finite; a program needn't handle non-finite values.
Results may differ from the reference program's by a relative error of at most 0.019.
Values may be sent and summed in bfloat16 or wider, within the bound.
A program may use at most 128 MiB of HBM per device.

```python
import jax
import jax.numpy as jnp
from jax import lax

D = 3584
RANK = 256
LAYERS = 2
STEPS = 4
TOK = 256
REPLICAS = 8


def draw_hidden(key, part):
    values = jax.random.truncated_normal(jax.random.fold_in(key, 11), -6.0, 6.0, (REPLICAS, TOK, D), jnp.float32)
    return values.astype(jnp.bfloat16)


def draw_target(key, part):
    values = jax.random.truncated_normal(jax.random.fold_in(key, 12), -6.0, 6.0, (REPLICAS, TOK, D), jnp.float32)
    return values.astype(jnp.bfloat16)


def draw_w_down(key, part):
    values = jax.random.truncated_normal(jax.random.fold_in(key, 13), -5.0, 5.0, (REPLICAS, LAYERS, D, RANK), jnp.float32)
    return values.astype(jnp.bfloat16)


def draw_w_up(key, part):
    values = jax.random.truncated_normal(jax.random.fold_in(key, 14), -5.0, 5.0, (REPLICAS, LAYERS, RANK, D), jnp.float32)
    return values.astype(jnp.bfloat16)


def draw_m_down(key, part):
    values = 1.5 * jax.random.truncated_normal(jax.random.fold_in(key, 15), -6.0, 6.0, (REPLICAS, LAYERS, D, RANK), jnp.float32)
    return values.astype(jnp.float32)


def draw_m_up(key, part):
    values = 1.5 * jax.random.truncated_normal(jax.random.fold_in(key, 16), -6.0, 6.0, (REPLICAS, LAYERS, RANK, D), jnp.float32)
    return values.astype(jnp.float32)


def setup_inputs(seed: int = 0) -> dict:
    seeds = jax.random.split(jax.random.key(seed), 7)
    return {
        "hidden": draw_hidden(jax.random.fold_in(seeds[6], 71), 0),
        "target": draw_target(jax.random.fold_in(seeds[6], 71), 0),
        "w_down": draw_w_down(jax.random.fold_in(seeds[6], 71), 0),
        "w_up": draw_w_up(jax.random.fold_in(seeds[6], 71), 0),
        "m_down": draw_m_down(jax.random.fold_in(seeds[6], 71), 0),
        "m_up": draw_m_up(jax.random.fold_in(seeds[6], 71), 0),
    }


norm_eps = 1e-06
learn_rate = 0.02
moment_decay = 0.9

def silu_slope(preact):
    sigmoid_v = jax.nn.sigmoid(preact)
    return sigmoid_v * (1.0 + preact * (1.0 - sigmoid_v))

def replica_steps(hidden, target, w_down, w_up, m_down, m_up):
    for step_index in range(STEPS):
        stored = []
        current = hidden
        for layer_index in range(LAYERS):
            wide_rows = current.astype(jnp.float32)
            root_mean = jnp.sqrt(lax.optimization_barrier(jnp.mean(wide_rows * wide_rows, axis=1, keepdims=True)) + norm_eps)
            projected = jnp.dot(current, w_down[layer_index], preferred_element_type=jnp.float32) * D ** (-0.5)
            preact = projected / root_mean
            activation = jax.nn.silu(preact).astype(jnp.bfloat16)
            stored.append((current, root_mean, preact, activation))
            lifted = jnp.dot(activation, w_up[layer_index], preferred_element_type=jnp.float32) * RANK ** (-0.5)
            current = (wide_rows + lifted).astype(jnp.bfloat16)
        gradient = current.astype(jnp.float32) - target.astype(jnp.float32)
        grads_down = [None] * LAYERS
        grads_up = [None] * LAYERS
        for layer_index in reversed(range(LAYERS)):
            current, root_mean, preact, activation = stored[layer_index]
            grad_low = gradient.astype(jnp.bfloat16)
            grads_up[layer_index] = jnp.dot(activation.T, grad_low, preferred_element_type=jnp.float32) * RANK ** (-0.5)
            grad_act = jnp.dot(grad_low, w_up[layer_index].T, preferred_element_type=jnp.float32) * RANK ** (-0.5)
            grad_pre = grad_act * silu_slope(preact)
            row_dot = lax.optimization_barrier(jnp.sum(grad_pre * preact, axis=1, keepdims=True))
            grad_proj = (grad_pre / root_mean).astype(jnp.bfloat16)
            grads_down[layer_index] = jnp.dot(current.T, grad_proj, preferred_element_type=jnp.float32) * D ** (-0.5)
            wide_rows = current.astype(jnp.float32)
            through = jnp.dot(grad_proj, w_down[layer_index].T, preferred_element_type=jnp.float32) * D ** (-0.5)
            gradient = gradient + through - row_dot * wide_rows / (D * root_mean * root_mean)
        m_down = moment_decay * m_down + jnp.stack(grads_down)
        m_up = moment_decay * m_up + jnp.stack(grads_up)
        w_down = (w_down.astype(jnp.float32) - learn_rate * m_down).astype(jnp.bfloat16)
        w_up = (w_up.astype(jnp.float32) - learn_rate * m_up).astype(jnp.bfloat16)
    return (w_down, w_up, m_down, m_up)

def accumulate(totals, inputs):
    finals = replica_steps(inputs[0], inputs[1], inputs[2], inputs[3], inputs[4], inputs[5])
    return (tuple((total + final.astype(jnp.float32) for total, final in zip(totals, finals))), None)

def reference(hidden, target, w_down, w_up, m_down, m_up):
    replicas = hidden.shape[0]
    zeros_init = (jnp.zeros(w_down.shape[1:], jnp.float32), jnp.zeros(w_up.shape[1:], jnp.float32), jnp.zeros(m_down.shape[1:], jnp.float32), jnp.zeros(m_up.shape[1:], jnp.float32))
    totals, unused = lax.scan(accumulate, zeros_init, (hidden, target, w_down, w_up, m_down, m_up))
    avg_down = (totals[0] / replicas).astype(jnp.bfloat16)
    avg_up = (totals[1] / replicas).astype(jnp.bfloat16)
    return (avg_down, avg_up, totals[2] / replicas, totals[3] / replicas)
```

```python
import functools

import jax
import jax.numpy as jnp
from jax import lax
from jax.experimental import pallas as pl
from jax.experimental.pallas import tpu as pltpu
from jax.sharding import PartitionSpec as P

MESH = pl.DeviceIdType.MESH
STEPS = 4
norm_eps = 1e-06
learn_rate = 0.02
moment_decay = 0.9


def dot_nn(a, b):
    return jnp.dot(a, b, preferred_element_type=jnp.float32)


def dot_nt(a, b):
    return lax.dot_general(a, b, (((1,), (1,)), ((), ())), preferred_element_type=jnp.float32)


def row_bits(replicas, *lengths):
    if replicas & (replicas - 1) or any(length % (16 * replicas) for length in lengths):
        return []
    return [2**k for k in range(replicas.bit_length() - 1)]


def fused_kernel(
    shards, replicas,
    x0_ref, tg_ref, wd_in, wu_in, md_in, mu_in,
    wd_out, wu_out, md_out, mu_out,
    wd, wu, md, mu, wdl, wul, mdl, mul, res_wd, res_wu, res_md, res_mu,
    got_wd, got_wu, got_md, got_mu, row_send, row_recv,
    x1, xt, gr, pre, act, inv, low, proj, slope, gram, sqs,
    s1, r1, s2, r2, s3, r3, tot, q1, p1, q2, p2, q3, p3,
    main_send, main_recv, side_send, side_recv,
):
    tok, width = x0_ref.shape
    rank = wd.shape[2]
    full = width * shards
    half = tok // 2
    chips = shards // 2
    me = lax.axis_index("ta")
    core = lax.rem(me, 2)
    sibling = me + 1 - 2 * core
    partners = [lax.rem(me + 2 * k, shards) for k in range(1, chips)]
    hops = chips - 1
    d_scale = full ** (-0.5)
    r_scale = rank ** (-0.5)

    barrier = pltpu.get_barrier_semaphore()
    for peer in [sibling] + partners:
        pl.semaphore_signal(barrier, inc=1, device_id={"ta": peer}, device_id_type=MESH)
    bits = row_bits(replicas, width, rank)
    levels = len(bits)
    spot = lax.axis_index("row")
    own_bit = {bit: lax.rem(spot // bit, 2) for bit in bits}
    row_peer = {bit: spot + bit - 2 * bit * own_bit[bit] for bit in bits}
    for bit in bits:
        pl.semaphore_signal(barrier, inc=1, device_id={"row": row_peer[bit]}, device_id_type=MESH)
    pl.semaphore_wait(barrier, chips + levels)

    wd[...] = wd_in[...]
    wu[...] = wu_in[...]
    md[...] = md_in[...]
    mu[...] = mu_in[...]

    def send(src, dst, sems, index, peer):
        copy = pltpu.make_async_remote_copy(
            src_ref=src, dst_ref=dst,
            send_sem=sems[0].at[index], recv_sem=sems[1].at[index],
            device_id={"ta": peer}, device_id_type=MESH,
        )
        copy.start()
        return copy

    main = (main_send, main_recv)
    side = (side_send, side_recv)
    per_channel = 2 + 2 * hops

    def to_row(column):
        return jnp.broadcast_to(column, (half, half)).T[0:8]

    def to_column(row):
        return jnp.broadcast_to(row[0:1, :], (half, half)).T[:, 0:1]

    class Channel:
        def __init__(self, which):
            self.which = which
            self.size = tot[which].shape[0] // 2
            size = self.size
            self.mine = pl.ds(pl.multiple_of(core * size, size), size)
            self.other = pl.ds(pl.multiple_of((1 - core) * size, size), size)
            self.base = which * per_channel

        def begin(self, parity, value, squares=None):
            c = self.which
            self.parity = parity
            self.squares = squares is not None
            tot[c][...] = value
            s1[c][...] = tot[c][self.other, :].astype(jnp.bfloat16)
            self.copies = [send(s1[c], r1[c], main, self.base, sibling)]
            if self.squares:
                sqs[...] = squares
                q1[...] = to_row(sqs[self.other, :])
                self.copies.append(send(q1, p1, side, 0, sibling))

        def cross(self):
            c = self.which
            for copy in self.copies:
                copy.wait()
            pair = tot[c][self.mine, :] + r1[c][...].astype(jnp.float32)
            s2[c][...] = pair.astype(jnp.bfloat16)
            spots = [self.parity * hops + k for k in range(hops)]
            self.copies = [
                send(s2[c], r2[c].at[spot], main, self.base + 2 + spot, peer)
                for spot, peer in zip(spots, partners)
            ]
            tot[c][self.mine, :] = pair
            if self.squares:
                self.row = to_row(sqs[self.mine, :]) + p1[...]
                q2[...] = self.row
                self.copies += [
                    send(q2, p2.at[spot], side, 2 + spot, peer)
                    for spot, peer in zip(spots, partners)
                ]

        def back(self):
            c = self.which
            for copy in self.copies:
                copy.wait()
            total = tot[c][self.mine, :]
            for k in range(hops):
                total = total + r2[c][self.parity * hops + k].astype(jnp.float32)
            s3[c][...] = total.astype(jnp.bfloat16)
            self.copies = [send(s3[c], r3[c], main, self.base + 1, sibling)]
            tot[c][self.mine, :] = total
            if self.squares:
                row = self.row
                for k in range(hops):
                    row = row + p2[self.parity * hops + k]
                q3[...] = row
                self.copies.append(send(q3, p3, side, 1, sibling))
                sqs[self.mine, :] = to_column(row)

        def end(self):
            c = self.which
            for copy in self.copies:
                copy.wait()
            tot[c][self.other, :] = r3[c][...].astype(jnp.float32)
            if self.squares:
                sqs[self.other, :] = to_column(p3[...])
            return tot[c][...]

    forth, own_act, low_act, cross_weight, low_input = [Channel(k) for k in range(5)]

    def update(w, m, layer, grad, last):
        moment = moment_decay * m[layer] + grad
        m[layer] = moment
        if last and levels:
            return
        w[layer] = (w[layer].astype(jnp.float32) - learn_rate * moment).astype(jnp.bfloat16)

    def update_up(layer, last):
        update(wu, mu, layer, dot_nn(act[layer].T, gr[...].astype(jnp.bfloat16)) * r_scale, last)

    def update_down(layer, rows_t, last):
        update(wd, md, layer, dot_nn(rows_t, low[layer]) * d_scale, last)

    def activate(layer, preact):
        activation = (preact * jax.nn.sigmoid(preact)).astype(jnp.bfloat16)
        pre[layer] = preact
        act[layer] = activation
        return activation

    def low_grads(layer, grad_act):
        preact = pre[layer]
        sig = jax.nn.sigmoid(preact)
        grad_pre = grad_act * (sig * (1.0 + preact * (1.0 - sig)))
        low[layer] = (grad_pre * inv[layer]).astype(jnp.bfloat16)
        return jnp.sum(grad_pre * preact, axis=1, keepdims=True)

    down, up = (wdl, got_wd, res_wd), (wul, got_wu, res_wu)
    mdown, mup = (mdl, got_md, res_md), (mul, got_mu, res_mu)
    layers = list(reversed(range(wd.shape[0])))
    chunks = [pair + (layer, bits) for layer in layers for pair in (up, down)]
    first = len(chunks)
    swapped = bits[:2][::-1] + bits[2:]
    chunks += [
        pair + (layer, swapped if layer == 0 and pair is mup else bits)
        for layer in layers
        for pair in (mup, mdown)
    ]

    def start(picked):
        for chunk in picked if levels else []:
            row_copy(chunk, 0).start()

    def advance(slot):
        for chunk in range(len(chunks)):
            stage = slot - chunk
            if not levels or stage < 0 or stage >= 2 * levels:
                continue
            row_copy(chunk, stage).wait_recv()
            if stage < levels:
                acc, got, res, layer, order = chunks[chunk]
                size = acc.shape[1] >> (stage + 1)
                keep = pl.ds(region(chunk, stage + 1), size)
                landed = got.at[layer, pl.ds(acc.shape[1] - 2 * size, size)]
                total = acc[layer, keep, :].astype(jnp.float32) + landed[...].astype(jnp.float32)
                if stage < levels - 1:
                    acc[layer, keep, :] = total.astype(jnp.bfloat16)
                else:
                    res[layer, keep, :] = (total * (1.0 / replicas)).astype(jnp.bfloat16)
            if stage < 2 * levels - 1:
                row_copy(chunk, stage + 1).start()

    def region(chunk, depth):
        acc, _, _, _, order = chunks[chunk]
        start = 0
        for k in range(depth):
            start = start + own_bit[order[k]] * (acc.shape[1] >> (k + 1))
        return pl.multiple_of(start, acc.shape[1] >> depth) if depth else 0

    def row_copy(chunk, stage):
        acc, got, res, layer, order = chunks[chunk]
        rows = acc.shape[1]
        if stage < levels:
            bit = order[stage]
            size = rows >> (stage + 1)
            away = region(chunk, stage) + (1 - own_bit[bit]) * size
            src = acc.at[layer, pl.ds(pl.multiple_of(away, size), size)]
            dst = got.at[layer, pl.ds(rows - 2 * size, size)]
        else:
            depth = 2 * levels - stage
            bit = order[depth - 1]
            part = pl.ds(region(chunk, depth), rows >> depth)
            src = dst = res.at[layer, part]
        index = chunk * 2 * levels + stage
        return pltpu.make_async_remote_copy(
            src_ref=src, dst_ref=dst,
            send_sem=row_send.at[index], recv_sem=row_recv.at[index],
            device_id={"row": row_peer[bit]}, device_id_type=MESH,
        )

    def step(parity, last, deferred):
        if last:
            wul[...] = wu[...]
            wdl[1] = wd[1]
            start(range(first - 1))
        activation = activate(0, proj[...] * inv[0])
        lifted = dot_nn(activation, wu[0]) * r_scale
        x1[...] = (x0_ref[...].astype(jnp.float32) + lifted).astype(jnp.bfloat16)
        wide = x1[...].astype(jnp.float32)
        squares = jnp.sum(wide * wide, axis=1, keepdims=True)
        forth.begin(parity, dot_nn(x1[...], wd[1]) * d_scale, squares)
        cross_weight.begin(parity, dot_nn(wu[0], wd[1]) * (r_scale * d_scale))
        forth.cross()
        low_input.begin(parity, dot_nt(x1[...], wu[0]) * r_scale)
        cross_weight.cross()
        low_input.cross()
        deferred()
        if last:
            wdl[0] = wd[0]
            start([first - 1])
            advance(0)
        forth.back()
        forth.end()
        inv[1] = lax.rsqrt(sqs[...] / full + norm_eps)
        activation = activate(1, tot[0][...] * inv[1])
        lifted = dot_nn(activation, wu[1]) * r_scale
        outcome = (x1[...].astype(jnp.float32) + lifted).astype(jnp.bfloat16)
        gr[...] = outcome.astype(jnp.float32) - tg_ref[...].astype(jnp.float32)
        grad_low = gr[...].astype(jnp.bfloat16)
        own_act.begin(parity, dot_nt(grad_low, wu[1]) * r_scale)
        low_act.begin(parity, dot_nt(grad_low, wu[0]) * r_scale)
        own_act.cross()
        low_act.cross()
        update_up(1, last)
        cross_weight.back()
        low_input.back()
        if last:
            advance(1)
        own_act.back()
        row_dot = low_grads(1, own_act.end())
        coefficient = row_dot * inv[1] * inv[1] / full
        through = dot_nt(low[1], wd[1]) * d_scale
        gr[...] = gr[...] + through - coefficient * x1[...].astype(jnp.float32)
        low_act.back()
        update_up(0, last)
        update_down(1, x1[...].T, last)
        weight = cross_weight.end().astype(jnp.bfloat16)
        grad_act = dot_nt(low[1], weight) - coefficient * low_input.end()
        low_grads(0, low_act.end() + grad_act)
        if last:
            return
        slope[...] = moment_decay * slope[...] + dot_nn(gram[...], low[0]) * (d_scale * d_scale)
        proj[...] = proj[...] - learn_rate * slope[...]

    def late_down(last=False):
        update_down(0, xt[...], last)

    def middle(index, carry):
        step(lax.rem(index, 2), False, lambda: pl.when(index > 0)(late_down))
        return carry

    xt[...] = x0_ref[...].T
    wide_input = x0_ref[...].astype(jnp.float32)
    squares = jnp.sum(wide_input * wide_input, axis=1, keepdims=True)
    forth.begin(1, dot_nn(x0_ref[...], wd[0]) * d_scale, squares)
    own_act.begin(1, dot_nn(x0_ref[...], md[0].astype(jnp.bfloat16)) * d_scale)
    low_act.begin(1, dot_nn(x0_ref[...], xt[...]))
    forth.cross()
    own_act.cross()
    low_act.cross()
    forth.back()
    own_act.back()
    low_act.back()
    proj[...] = forth.end()
    inv[0] = lax.rsqrt(sqs[...] / full + norm_eps)
    slope[...] = own_act.end()
    gram[...] = low_act.end().astype(jnp.bfloat16)
    lax.fori_loop(0, STEPS - 1, middle, 0)
    step((STEPS - 1) % 2, True, late_down)
    if levels:
        mul[...] = mu[...].astype(jnp.bfloat16)
        mdl[1] = md[1].astype(jnp.bfloat16)
        start(range(first, len(chunks) - 1))
    late_down(True)
    mdl[0] = md[0].astype(jnp.bfloat16)
    if not levels:
        mul[...] = mu[...].astype(jnp.bfloat16)
        mdl[1] = md[1].astype(jnp.bfloat16)
    if not levels:
        wd_out[...] = wd[...]
        wu_out[...] = wu[...]
        md_out[...] = mdl[...]
        mu_out[...] = mul[...]
        return
    start([len(chunks) - 1])
    for slot in range(2, len(chunks) + 2 * levels - 1):
        advance(slot)
    for chunk in range(len(chunks)):
        for stage in range(2 * levels):
            row_copy(chunk, stage).wait_send()

    def stepped(weights, moments):
        moved = weights.astype(jnp.float32) - learn_rate * moments.astype(jnp.float32)
        return moved.astype(jnp.bfloat16)

    wd_out[...] = stepped(res_wd[...], res_md[...])
    wu_out[...] = stepped(res_wu[...], res_mu[...])
    md_out[...] = res_md[...]
    mu_out[...] = res_mu[...]


def fused(shards, replicas, hidden, target, w_down, w_up, m_down, m_up):
    tok, width = hidden.shape
    layers, _, rank = w_down.shape
    half = tok // 2
    hops = shards // 2 - 1
    bf, f32 = jnp.bfloat16, jnp.float32
    vmem = pl.BlockSpec(memory_space=pltpu.VMEM)
    channels = 5
    sems = channels * (2 + 2 * hops)
    rows = [tok, tok, tok, rank, tok]
    halves = [pltpu.VMEM((count // 2, rank), bf) for count in rows]
    crossed = [pltpu.VMEM((2 * hops, count // 2, rank), bf) for count in rows]
    totals = [pltpu.VMEM((count, rank), f32) for count in rows]
    row_sems = max(1, 4 * layers * 2 * len(row_bits(replicas, width, rank)))
    return pl.pallas_call(
        functools.partial(fused_kernel, shards, replicas),
        out_shape=[
            jax.ShapeDtypeStruct(w_down.shape, bf),
            jax.ShapeDtypeStruct(w_up.shape, bf),
            jax.ShapeDtypeStruct(m_down.shape, bf),
            jax.ShapeDtypeStruct(m_up.shape, bf),
        ],
        in_specs=[vmem] * 6,
        out_specs=[vmem] * 4,
        scratch_shapes=[
            pltpu.VMEM(w_down.shape, bf),
            pltpu.VMEM(w_up.shape, bf),
            pltpu.VMEM(m_down.shape, f32),
            pltpu.VMEM(m_up.shape, f32),
            pltpu.VMEM(w_down.shape, bf),
            pltpu.VMEM(w_up.shape, bf),
            pltpu.VMEM(m_down.shape, bf),
            pltpu.VMEM(m_up.shape, bf),
            pltpu.VMEM(w_down.shape, bf),
            pltpu.VMEM(w_up.shape, bf),
            pltpu.VMEM(m_down.shape, bf),
            pltpu.VMEM(m_up.shape, bf),
            pltpu.VMEM(w_down.shape, bf),
            pltpu.VMEM(w_up.shape, bf),
            pltpu.VMEM(m_down.shape, bf),
            pltpu.VMEM(m_up.shape, bf),
            pltpu.SemaphoreType.DMA((row_sems,)),
            pltpu.SemaphoreType.DMA((row_sems,)),
            pltpu.VMEM((tok, width), bf),
            pltpu.VMEM((width, tok), bf),
            pltpu.VMEM((tok, width), f32),
            pltpu.VMEM((layers, tok, rank), f32),
            pltpu.VMEM((layers, tok, rank), bf),
            pltpu.VMEM((layers, tok, 1), f32),
            pltpu.VMEM((layers, tok, rank), bf),
            pltpu.VMEM((tok, rank), f32),
            pltpu.VMEM((tok, rank), f32),
            pltpu.VMEM((tok, tok), bf),
            pltpu.VMEM((tok, 1), f32),
            halves,
            halves,
            halves,
            crossed,
            halves,
            halves,
            totals,
            pltpu.VMEM((8, half), f32),
            pltpu.VMEM((8, half), f32),
            pltpu.VMEM((8, half), f32),
            pltpu.VMEM((2 * hops, 8, half), f32),
            pltpu.VMEM((8, half), f32),
            pltpu.VMEM((8, half), f32),
            pltpu.SemaphoreType.DMA((sems,)),
            pltpu.SemaphoreType.DMA((sems,)),
            pltpu.SemaphoreType.DMA((2 + 2 * hops,)),
            pltpu.SemaphoreType.DMA((2 + 2 * hops,)),
        ],
        compiler_params=pltpu.CompilerParams(
            collective_id=0, has_side_effects=True, vmem_limit_bytes=60 * 1024 * 1024
        ),
    )(hidden, target, w_down, w_up, m_down, m_up)


def body(shards, replicas, hidden, target, w_down, w_up, m_down, m_up):
    means = fused(
        shards, replicas, hidden[0], target[0], w_down[0], w_up[0], m_down[0], m_up[0]
    )
    if not row_bits(replicas, hidden.shape[2], w_down.shape[3]):
        totals = lax.psum(tuple(means), "row")
        means = [total.astype(jnp.float32) / replicas for total in totals]
    return (
        means[0].astype(jnp.bfloat16),
        means[1].astype(jnp.bfloat16),
        means[2].astype(jnp.float32),
        means[3].astype(jnp.float32),
    )


def solution(mesh):
    placed = (
        P("row", None, "ta"),
        P("row", None, "ta"),
        P("row", None, "ta", None),
        P("row", None, None, "ta"),
        P("row", None, "ta", None),
        P("row", None, None, "ta"),
    )
    return jax.shard_map(
        functools.partial(body, mesh.shape["ta"], mesh.shape["row"]),
        mesh=mesh,
        in_specs=placed,
        out_specs=(
            P(None, "ta", None),
            P(None, None, "ta"),
            P(None, "ta", None),
            P(None, None, "ta"),
        ),
        check_vma=False,
    )
```

```python
import functools

import jax
import jax.numpy as jnp
from jax import lax
from jax.experimental import pallas as pl
from jax.experimental.pallas import tpu as pltpu
from jax.sharding import PartitionSpec as P

MESH = pl.DeviceIdType.MESH
STEPS = 4
norm_eps = 1e-06
learn_rate = 0.02
moment_decay = 0.9


def dot_nn(a, b):
    return jnp.dot(a, b, preferred_element_type=jnp.float32)


def dot_nt(a, b):
    return lax.dot_general(a, b, (((1,), (1,)), ((), ())), preferred_element_type=jnp.float32)


LINES = 4
FOLD_PARTS, LINE_PARTS = 5, 2
KINDS = 6


def on_grid(replicas, width, rank):
    return replicas == 2 * LINES and width % 128 == 0 and rank % 128 == 0 and width >= 512


def cuts(length, wide):
    if not wide:
        return [("fold", k * (length // 2), length // 2) for k in range(2)]
    line = length * LINE_PARTS // (FOLD_PARTS + LINE_PARTS) // 128 * 128
    return [("line", 0, line), ("fold", line, length - line)]


def fused_kernel(
    shards, replicas,
    x0_ref, tg_ref, wd_in, wu_in, md_in, mu_in,
    wd_out, wu_out, md_out, mu_out,
    wd, wu, md, mu, wdl, wul, mdl, mul, res_wd, res_wu, res_md, res_mu,
    got_wd, got_wu, got_md, got_mu, row_send, row_recv,
    x1, xt, gr, pre, act, inv, low, proj, slope, gram, sqs,
    s1, r1, s2, r2, s3, r3, tot, q1, p1, q2, p2, q3, p3,
    main_send, main_recv, side_send, side_recv,
):
    tok, width = x0_ref.shape
    rank = wd.shape[2]
    full = width * shards
    half = tok // 2
    chips = shards // 2
    me = lax.axis_index("ta")
    core = lax.rem(me, 2)
    sibling = me + 1 - 2 * core
    partners = [lax.rem(me + 2 * k, shards) for k in range(1, chips)]
    hops = chips - 1
    d_scale = full ** (-0.5)
    r_scale = rank ** (-0.5)

    barrier = pltpu.get_barrier_semaphore()
    for peer in [sibling] + partners:
        pl.semaphore_signal(barrier, inc=1, device_id={"ta": peer}, device_id_type=MESH)
    levels = on_grid(replicas, width, rank)
    spot = lax.axis_index("row")
    line, side_of = spot // 2, lax.rem(spot, 2)
    facing = spot + 1 - 2 * side_of
    after, before = lax.rem(spot + 2, replicas), lax.rem(spot + replicas - 2, replicas)
    greeted = [facing, after, before] if levels else []
    for peer in greeted:
        pl.semaphore_signal(barrier, inc=1, device_id={"row": peer}, device_id_type=MESH)
    pl.semaphore_wait(barrier, chips + len(greeted))

    wd[...] = wd_in[...]
    wu[...] = wu_in[...]
    md[...] = md_in[...]
    mu[...] = mu_in[...]

    def send(src, dst, sems, index, peer):
        copy = pltpu.make_async_remote_copy(
            src_ref=src, dst_ref=dst,
            send_sem=sems[0].at[index], recv_sem=sems[1].at[index],
            device_id={"ta": peer}, device_id_type=MESH,
        )
        copy.start()
        return copy

    main = (main_send, main_recv)
    side = (side_send, side_recv)
    per_channel = 2 + 2 * hops

    def to_row(column):
        return jnp.broadcast_to(column, (half, half)).T[0:8]

    def to_column(row):
        return jnp.broadcast_to(row[0:1, :], (half, half)).T[:, 0:1]

    class Channel:
        def __init__(self, which):
            self.which = which
            self.size = tot[which].shape[0] // 2
            size = self.size
            self.mine = pl.ds(pl.multiple_of(core * size, size), size)
            self.other = pl.ds(pl.multiple_of((1 - core) * size, size), size)
            self.base = which * per_channel

        def begin(self, parity, value, squares=None):
            c = self.which
            self.parity = parity
            self.squares = squares is not None
            tot[c][...] = value
            s1[c][...] = tot[c][self.other, :].astype(jnp.bfloat16)
            self.copies = [send(s1[c], r1[c], main, self.base, sibling)]
            if self.squares:
                sqs[...] = squares
                q1[...] = to_row(sqs[self.other, :])
                self.copies.append(send(q1, p1, side, 0, sibling))

        def cross(self):
            c = self.which
            for copy in self.copies:
                copy.wait()
            pair = tot[c][self.mine, :] + r1[c][...].astype(jnp.float32)
            s2[c][...] = pair.astype(jnp.bfloat16)
            spots = [self.parity * hops + k for k in range(hops)]
            self.copies = [
                send(s2[c], r2[c].at[spot], main, self.base + 2 + spot, peer)
                for spot, peer in zip(spots, partners)
            ]
            tot[c][self.mine, :] = pair
            if self.squares:
                self.row = to_row(sqs[self.mine, :]) + p1[...]
                q2[...] = self.row
                self.copies += [
                    send(q2, p2.at[spot], side, 2 + spot, peer)
                    for spot, peer in zip(spots, partners)
                ]

        def back(self):
            c = self.which
            for copy in self.copies:
                copy.wait()
            total = tot[c][self.mine, :]
            for k in range(hops):
                total = total + r2[c][self.parity * hops + k].astype(jnp.float32)
            s3[c][...] = total.astype(jnp.bfloat16)
            self.copies = [send(s3[c], r3[c], main, self.base + 1, sibling)]
            tot[c][self.mine, :] = total
            if self.squares:
                row = self.row
                for k in range(hops):
                    row = row + p2[self.parity * hops + k]
                q3[...] = row
                self.copies.append(send(q3, p3, side, 1, sibling))
                sqs[self.mine, :] = to_column(row)

        def end(self):
            c = self.which
            for copy in self.copies:
                copy.wait()
            tot[c][self.other, :] = r3[c][...].astype(jnp.float32)
            if self.squares:
                sqs[self.other, :] = to_column(p3[...])
            return tot[c][...]

    forth, own_act, low_act, cross_weight, low_input = [Channel(k) for k in range(5)]

    def update(w, m, layer, grad, last):
        moment = moment_decay * m[layer] + grad
        m[layer] = moment
        if last and levels:
            return
        w[layer] = (w[layer].astype(jnp.float32) - learn_rate * moment).astype(jnp.bfloat16)

    def update_up(layer, last):
        update(wu, mu, layer, dot_nn(act[layer].T, gr[...].astype(jnp.bfloat16)) * r_scale, last)

    def update_down(layer, rows_t, last):
        update(wd, md, layer, dot_nn(rows_t, low[layer]) * d_scale, last)

    def activate(layer, preact):
        activation = (preact * jax.nn.sigmoid(preact)).astype(jnp.bfloat16)
        pre[layer] = preact
        act[layer] = activation
        return activation

    def low_grads(layer, grad_act):
        preact = pre[layer]
        sig = jax.nn.sigmoid(preact)
        grad_pre = grad_act * (sig * (1.0 + preact * (1.0 - sig)))
        low[layer] = (grad_pre * inv[layer]).astype(jnp.bfloat16)
        return jnp.sum(grad_pre * preact, axis=1, keepdims=True)

    down, up = (wdl, got_wd, res_wd), (wul, got_wu, res_wu)
    mdown, mup = (mdl, got_md, res_md), (mul, got_mu, res_mu)
    layers = list(reversed(range(wd.shape[0])))
    chunks = []
    for pairs in ((up, down), (mup, mdown)):
        for layer in layers:
            for pair, wide in zip(pairs, (False, True)):
                for form, base, size in cuts(pair[0].shape[1], wide):
                    chunks.append((pair, layer, form, base, size))
    first = len(chunks) // 2
    part = first // 4
    sent = []

    class Piece:
        def __init__(self, index):
            (self.acc, self.got, self.res), self.layer, self.form, self.base, self.size = chunks[index]
            self.index = index
            self.stages = 7 if self.form == "fold" else 9

        def rows(self, ref, start, size, slot=0):
            first_row = self.base + (slot - 1 if slot else 0) * self.acc.shape[1]
            start = start + first_row
            if not isinstance(start, int):
                start = pl.multiple_of(start, 16)
            return ref.at[self.layer, pl.ds(start, size)]

        def copy(self, kind, src, dst, peer):
            index = self.index * KINDS + kind
            return pltpu.make_async_remote_copy(
                src_ref=src, dst_ref=dst,
                send_sem=row_send.at[index], recv_sem=row_recv.at[index],
                device_id={"row": peer}, device_id_type=MESH,
            )

        def sum_out(self, kind, start, size, slot, landing, peer, when=None):
            def go(finish=False):
                made = self.copy(
                    kind, self.rows(self.acc, start, size), self.rows(self.got, landing, size, slot), peer
                )
                made.wait_send() if finish else made.start()

            go()
            sent.append((when, functools.partial(go, True)))

        def mean_out(self, kind, start, size, peer, when=None):
            def go(finish=False):
                where = self.rows(self.res, start, size)
                made = self.copy(kind, where, where, peer)
                made.wait_send() if finish else made.start()

            go()
            sent.append((when, functools.partial(go, True)))

        def landed(self, kind, start, size, slot=0):
            ref = self.rows(self.got, start, size, slot) if slot else self.rows(self.res, start, size)
            self.copy(kind, ref, ref, facing).wait_recv()

        def add(self, start, size, slot, landing):
            mine = self.rows(self.acc, start, size)
            came = self.rows(self.got, landing, size, slot)
            total = mine[...].astype(jnp.float32) + came[...].astype(jnp.float32)
            mine[...] = total.astype(jnp.bfloat16)

        def settle(self, start, size, slot, landing):
            mine = self.rows(self.acc, start, size)
            came = self.rows(self.got, landing, size, slot)
            total = mine[...].astype(jnp.float32) + came[...].astype(jnp.float32)
            self.rows(self.res, start, size)[...] = (total * (1.0 / replicas)).astype(jnp.bfloat16)

        def run(self, stage):
            (self.fold if self.form == "fold" else self.line)(stage)

        def fold(self, stage):
            half_size, quarter = self.size // 2, self.size // 4
            keep, away = side_of * half_size, (1 - side_of) * half_size
            outer = (line == 0) | (line == LINES - 1)
            inner = jnp.logical_not(outer)
            upper = lax.rem(line // 2, 2)
            inward = spot + 2 - 4 * upper
            outward = spot - 2 + 4 * upper
            across = spot + 2 - 4 * upper
            own = keep + upper * quarter
            far = keep + (1 - upper) * quarter
            if stage == 0:
                self.sum_out(0, away, half_size, 1, 0, facing)
            elif stage == 1:
                self.landed(0, 0, half_size, 1)
                self.add(keep, half_size, 1, 0)

                @pl.when(outer)
                def _():
                    self.sum_out(1, keep, half_size, 2, 0, inward, outer)
            elif stage == 2:

                @pl.when(inner)
                def _():
                    self.landed(1, 0, half_size, 2)
                    self.add(keep, half_size, 2, 0)
                    self.sum_out(2, far, quarter, 3, 0, across, inner)
            elif stage == 3:

                @pl.when(inner)
                def _():
                    self.landed(2, 0, quarter, 3)
                    self.settle(own, quarter, 3, 0)
                    self.mean_out(3, own, quarter, across, inner)
            elif stage == 4:

                @pl.when(inner)
                def _():
                    self.landed(3, far, quarter)
                    self.mean_out(4, keep, half_size, outward, inner)
                    self.mean_out(5, keep, half_size, facing, inner)
            elif stage == 5:

                @pl.when(outer)
                def _():
                    self.landed(4, keep, half_size)
                    self.mean_out(5, keep, half_size, facing, outer)
            else:
                self.landed(5, away, half_size)

        def line(self, stage):
            piece = self.size // LINES
            fine = piece // 2
            end = LINES - 1
            if stage <= end:
                for at, step_to, kind, slot in ((stage, 1, 0, 1), (end - stage, -1, 1, 2)):
                    ahead = (at + 1) * piece if step_to > 0 else 0
                    count = (end - at) * piece if step_to > 0 else at * piece
                    came = (LINES - at) * piece if step_to > 0 else (at + 1) * piece
                    opened = at * piece if step_to > 0 else 0
                    here = line == at

                    @pl.when(here)
                    def _(ahead=ahead, count=count, came=came, opened=opened, kind=kind, slot=slot, here=here, peer=after if step_to > 0 else before):
                        if stage:
                            self.landed(kind, opened, came, slot)
                        if count:
                            if stage:
                                self.add(ahead, count, slot, ahead)
                            self.sum_out(kind, ahead, count, slot, ahead, peer, here)
            if stage == end:
                own = line * piece

                @pl.when(line > 0)
                def _():
                    self.add(own, piece, 1, own)

                @pl.when(line < end)
                def _():
                    self.add(own, piece, 2, own)

                self.sum_out(2, own + (1 - side_of) * fine, fine, 3, 0, facing)
            elif stage == end + 1:
                own = line * piece + side_of * fine
                self.landed(2, 0, fine, 3)
                self.settle(own, fine, 3, 0)
                self.mean_out(3, own, fine, facing)
            elif stage > end + 1:
                hop = stage - end - 2
                if hop == 0:
                    self.landed(3, line * piece + (1 - side_of) * fine, fine)
                for at, step_to, kind in ((hop, 1, 4), (end - hop, -1, 5)):
                    here = line == at
                    came = hop * piece
                    opened = 0 if step_to > 0 else (at + 1) * piece
                    begun = 0 if step_to > 0 else at * piece

                    @pl.when(here)
                    def _(came=came, opened=opened, begun=begun, kind=kind, here=here, peer=after if step_to > 0 else before):
                        if hop:
                            self.landed(kind, opened, came)
                        if hop < end:
                            self.mean_out(kind, begun, came + piece, peer, here)

    pieces = [Piece(k) for k in range(len(chunks))] if levels else []
    done = {k: 0 for k in range(len(chunks))}
    plan = sorted(
        (0.25 * (k % first) + (2.0 if k >= first else 0.0) + stage, k, stage)
        for k, piece in enumerate(pieces)
        for stage in range(1, piece.stages)
    )

    def start(picked):
        for k in picked if levels else []:
            pieces[k].run(0)

    def advance(count=None, below=None):
        taken = 0
        for entry in list(plan):
            if taken == count:
                break
            if below is not None and entry[1] >= below:
                continue
            pieces[entry[1]].run(entry[2])
            plan.remove(entry)
            taken += 1

    def step(parity, last, deferred):
        if last:
            wul[...] = wu[...]
            wdl[1] = wd[1]
            start(range(first - part))
        activation = activate(0, proj[...] * inv[0])
        lifted = dot_nn(activation, wu[0]) * r_scale
        x1[...] = (x0_ref[...].astype(jnp.float32) + lifted).astype(jnp.bfloat16)
        wide = x1[...].astype(jnp.float32)
        squares = jnp.sum(wide * wide, axis=1, keepdims=True)
        forth.begin(parity, dot_nn(x1[...], wd[1]) * d_scale, squares)
        cross_weight.begin(parity, dot_nn(wu[0], wd[1]) * (r_scale * d_scale))
        forth.cross()
        low_input.begin(parity, dot_nt(x1[...], wu[0]) * r_scale)
        cross_weight.cross()
        low_input.cross()
        deferred()
        if last:
            wdl[0] = wd[0]
            start(range(first - part, first))
            advance(4, first)
        forth.back()
        forth.end()
        inv[1] = lax.rsqrt(sqs[...] / full + norm_eps)
        activation = activate(1, tot[0][...] * inv[1])
        lifted = dot_nn(activation, wu[1]) * r_scale
        outcome = (x1[...].astype(jnp.float32) + lifted).astype(jnp.bfloat16)
        gr[...] = outcome.astype(jnp.float32) - tg_ref[...].astype(jnp.float32)
        grad_low = gr[...].astype(jnp.bfloat16)
        own_act.begin(parity, dot_nt(grad_low, wu[1]) * r_scale)
        low_act.begin(parity, dot_nt(grad_low, wu[0]) * r_scale)
        own_act.cross()
        low_act.cross()
        update_up(1, last)
        cross_weight.back()
        low_input.back()
        if last:
            advance(6, first)
        own_act.back()
        row_dot = low_grads(1, own_act.end())
        coefficient = row_dot * inv[1] * inv[1] / full
        through = dot_nt(low[1], wd[1]) * d_scale
        gr[...] = gr[...] + through - coefficient * x1[...].astype(jnp.float32)
        low_act.back()
        update_up(0, last)
        update_down(1, x1[...].T, last)
        weight = cross_weight.end().astype(jnp.bfloat16)
        grad_act = dot_nt(low[1], weight) - coefficient * low_input.end()
        low_grads(0, low_act.end() + grad_act)
        if last:
            return
        slope[...] = moment_decay * slope[...] + dot_nn(gram[...], low[0]) * (d_scale * d_scale)
        proj[...] = proj[...] - learn_rate * slope[...]

    def late_down(last=False):
        update_down(0, xt[...], last)

    def middle(index, carry):
        step(lax.rem(index, 2), False, lambda: pl.when(index > 0)(late_down))
        return carry

    xt[...] = x0_ref[...].T
    wide_input = x0_ref[...].astype(jnp.float32)
    squares = jnp.sum(wide_input * wide_input, axis=1, keepdims=True)
    forth.begin(1, dot_nn(x0_ref[...], wd[0]) * d_scale, squares)
    own_act.begin(1, dot_nn(x0_ref[...], md[0].astype(jnp.bfloat16)) * d_scale)
    low_act.begin(1, dot_nn(x0_ref[...], xt[...]))
    forth.cross()
    own_act.cross()
    low_act.cross()
    forth.back()
    own_act.back()
    low_act.back()
    proj[...] = forth.end()
    inv[0] = lax.rsqrt(sqs[...] / full + norm_eps)
    slope[...] = own_act.end()
    gram[...] = low_act.end().astype(jnp.bfloat16)
    lax.fori_loop(0, STEPS - 1, middle, 0)
    step((STEPS - 1) % 2, True, late_down)
    if levels:
        mul[...] = mu[...].astype(jnp.bfloat16)
        mdl[1] = md[1].astype(jnp.bfloat16)
        start(range(first, len(chunks) - part))
    late_down(True)
    mdl[0] = md[0].astype(jnp.bfloat16)
    if not levels:
        mul[...] = mu[...].astype(jnp.bfloat16)
        mdl[1] = md[1].astype(jnp.bfloat16)
    if not levels:
        wd_out[...] = wd[...]
        wu_out[...] = wu[...]
        md_out[...] = mdl[...]
        mu_out[...] = mul[...]
        return
    start(range(len(chunks) - part, len(chunks)))
    advance()
    for when, finish in sent:
        if when is None:
            finish()
        else:
            pl.when(when)(finish)

    def stepped(weights, moments):
        moved = weights.astype(jnp.float32) - learn_rate * moments.astype(jnp.float32)
        return moved.astype(jnp.bfloat16)

    wd_out[...] = stepped(res_wd[...], res_md[...])
    wu_out[...] = stepped(res_wu[...], res_mu[...])
    md_out[...] = res_md[...]
    mu_out[...] = res_mu[...]


def fused(shards, replicas, hidden, target, w_down, w_up, m_down, m_up):
    tok, width = hidden.shape
    layers, _, rank = w_down.shape
    half = tok // 2
    hops = shards // 2 - 1
    bf, f32 = jnp.bfloat16, jnp.float32
    vmem = pl.BlockSpec(memory_space=pltpu.VMEM)
    channels = 5
    sems = channels * (2 + 2 * hops)
    rows = [tok, tok, tok, rank, tok]
    halves = [pltpu.VMEM((count // 2, rank), bf) for count in rows]
    crossed = [pltpu.VMEM((2 * hops, count // 2, rank), bf) for count in rows]
    totals = [pltpu.VMEM((count, rank), f32) for count in rows]
    row_sems = 8 * layers * KINDS
    tripled = [(layers, 3 * count, other) for count, other in (w_down.shape[1:], w_up.shape[1:])] * 2
    return pl.pallas_call(
        functools.partial(fused_kernel, shards, replicas),
        out_shape=[
            jax.ShapeDtypeStruct(w_down.shape, bf),
            jax.ShapeDtypeStruct(w_up.shape, bf),
            jax.ShapeDtypeStruct(m_down.shape, bf),
            jax.ShapeDtypeStruct(m_up.shape, bf),
        ],
        in_specs=[vmem] * 6,
        out_specs=[vmem] * 4,
        scratch_shapes=[
            pltpu.VMEM(w_down.shape, bf),
            pltpu.VMEM(w_up.shape, bf),
            pltpu.VMEM(m_down.shape, f32),
            pltpu.VMEM(m_up.shape, f32),
            pltpu.VMEM(w_down.shape, bf),
            pltpu.VMEM(w_up.shape, bf),
            pltpu.VMEM(m_down.shape, bf),
            pltpu.VMEM(m_up.shape, bf),
            pltpu.VMEM(w_down.shape, bf),
            pltpu.VMEM(w_up.shape, bf),
            pltpu.VMEM(m_down.shape, bf),
            pltpu.VMEM(m_up.shape, bf),
            pltpu.VMEM(tripled[0], bf),
            pltpu.VMEM(tripled[1], bf),
            pltpu.VMEM(tripled[2], bf),
            pltpu.VMEM(tripled[3], bf),
            pltpu.SemaphoreType.DMA((row_sems,)),
            pltpu.SemaphoreType.DMA((row_sems,)),
            pltpu.VMEM((tok, width), bf),
            pltpu.VMEM((width, tok), bf),
            pltpu.VMEM((tok, width), f32),
            pltpu.VMEM((layers, tok, rank), f32),
            pltpu.VMEM((layers, tok, rank), bf),
            pltpu.VMEM((layers, tok, 1), f32),
            pltpu.VMEM((layers, tok, rank), bf),
            pltpu.VMEM((tok, rank), f32),
            pltpu.VMEM((tok, rank), f32),
            pltpu.VMEM((tok, tok), bf),
            pltpu.VMEM((tok, 1), f32),
            halves,
            halves,
            halves,
            crossed,
            halves,
            halves,
            totals,
            pltpu.VMEM((8, half), f32),
            pltpu.VMEM((8, half), f32),
            pltpu.VMEM((8, half), f32),
            pltpu.VMEM((2 * hops, 8, half), f32),
            pltpu.VMEM((8, half), f32),
            pltpu.VMEM((8, half), f32),
            pltpu.SemaphoreType.DMA((sems,)),
            pltpu.SemaphoreType.DMA((sems,)),
            pltpu.SemaphoreType.DMA((2 + 2 * hops,)),
            pltpu.SemaphoreType.DMA((2 + 2 * hops,)),
        ],
        compiler_params=pltpu.CompilerParams(
            collective_id=0, has_side_effects=True, vmem_limit_bytes=60 * 1024 * 1024
        ),
    )(hidden, target, w_down, w_up, m_down, m_up)


def body(shards, replicas, hidden, target, w_down, w_up, m_down, m_up):
    means = fused(
        shards, replicas, hidden[0], target[0], w_down[0], w_up[0], m_down[0], m_up[0]
    )
    if not on_grid(replicas, hidden.shape[2], w_down.shape[3]):
        totals = lax.psum(tuple(means), "row")
        means = [total.astype(jnp.float32) / replicas for total in totals]
    return (
        means[0].astype(jnp.bfloat16),
        means[1].astype(jnp.bfloat16),
        means[2].astype(jnp.float32),
        means[3].astype(jnp.float32),
    )


def solution(mesh):
    placed = (
        P("row", None, "ta"),
        P("row", None, "ta"),
        P("row", None, "ta", None),
        P("row", None, None, "ta"),
        P("row", None, "ta", None),
        P("row", None, None, "ta"),
    )
    return jax.shard_map(
        functools.partial(body, mesh.shape["ta"], mesh.shape["row"]),
        mesh=mesh,
        in_specs=placed,
        out_specs=(
            P(None, "ta", None),
            P(None, None, "ta"),
            P(None, "ta", None),
            P(None, None, "ta"),
        ),
        check_vma=False,
    )
```

```python
import functools

import jax
import jax.numpy as jnp
from jax import lax
from jax.experimental import pallas as pl
from jax.experimental.pallas import tpu as pltpu
from jax.sharding import PartitionSpec as P

MESH = pl.DeviceIdType.MESH
STEPS = 4
norm_eps = 1e-06
learn_rate = 0.02
moment_decay = 0.9


def dot_nn(a, b):
    return jnp.dot(a, b, preferred_element_type=jnp.float32)


def dot_nt(a, b):
    return lax.dot_general(a, b, (((1,), (1,)), ((), ())), preferred_element_type=jnp.float32)


LINES = 4
FOLD_PARTS, LINE_PARTS = 5, 2
KINDS = 6


def on_grid(replicas, width, rank):
    return replicas == 2 * LINES and width % 128 == 0 and rank % 128 == 0 and width >= 512


def cuts(length, wide):
    if not wide:
        return [("fold", k * (length // 2), length // 2) for k in range(2)]
    line = length * LINE_PARTS // (FOLD_PARTS + LINE_PARTS) // 128 * 128
    return [("line", 0, line), ("fold", line, length - line)]


def fused_kernel(
    shards, replicas,
    x0_in, tg_in, wd_in, wu_in, md_in, mu_in,
    wd_out, wu_out, md_out, mu_out,
    x0_ref, tg_ref, wd, wu, md, mu, load_sem, store_sem, wdl, wul, mdl, mul, res_wd, res_wu, res_md, res_mu,
    got_wd, got_wu, got_md, got_mu, row_send, row_recv,
    x1, x1t, xt, gr, pre, act, inv, low, proj, slope, gram, sqs,
    s1, r1, s2, r2, s3, r3, tot, q1, p1, q2, p2, q3, p3,
    main_send, main_recv, side_send, side_recv,
):
    tok, width = x0_ref.shape
    rank = wd.shape[2]
    loads = [
        pltpu.make_async_copy(source, target, load_sem.at[k])
        for k, (source, target) in enumerate((
            (x0_in, x0_ref), (wd_in, wd), (md_in, md), (wu_in, wu), (tg_in, tg_ref), (mu_in, mu),
        ))
    ]
    for load in loads:
        load.start()
    full = width * shards
    half = tok // 2
    chips = shards // 2
    me = lax.axis_index("ta")
    core = lax.rem(me, 2)
    sibling = me + 1 - 2 * core
    partners = [lax.rem(me + 2 * k, shards) for k in range(1, chips)]
    hops = chips - 1
    d_scale = full ** (-0.5)
    r_scale = rank ** (-0.5)

    barrier = pltpu.get_barrier_semaphore()
    for peer in [sibling] + partners:
        pl.semaphore_signal(barrier, inc=1, device_id={"ta": peer}, device_id_type=MESH)
    levels = on_grid(replicas, width, rank)
    spot = lax.axis_index("row")
    line, side_of = spot // 2, lax.rem(spot, 2)
    facing = spot + 1 - 2 * side_of
    after, before = lax.rem(spot + 2, replicas), lax.rem(spot + replicas - 2, replicas)
    greeted = [facing, after, before] if levels else []
    for peer in greeted:
        pl.semaphore_signal(barrier, inc=1, device_id={"row": peer}, device_id_type=MESH)
    pl.semaphore_wait(barrier, chips + len(greeted))

    def send(src, dst, sems, index, peer):
        copy = pltpu.make_async_remote_copy(
            src_ref=src, dst_ref=dst,
            send_sem=sems[0].at[index], recv_sem=sems[1].at[index],
            device_id={"ta": peer}, device_id_type=MESH,
        )
        copy.start()
        return copy

    main = (main_send, main_recv)
    side = (side_send, side_recv)
    per_channel = 2 + 2 * hops

    def to_row(column):
        return jnp.broadcast_to(column, (half, half)).T[0:8]

    def to_column(row):
        return jnp.broadcast_to(row[0:1, :], (half, half)).T[:, 0:1]

    class Channel:
        def __init__(self, which):
            self.which = which
            self.size = tot[which].shape[0] // 2
            size = self.size
            self.mine = pl.ds(pl.multiple_of(core * size, size), size)
            self.other = pl.ds(pl.multiple_of((1 - core) * size, size), size)
            self.base = which * per_channel

        def begin(self, parity, value, squares=None):
            c = self.which
            self.parity = parity
            self.squares = squares is not None
            tot[c][...] = value
            s1[c][...] = tot[c][self.other, :].astype(jnp.bfloat16)
            self.copies = [send(s1[c], r1[c], main, self.base, sibling)]
            if self.squares:
                sqs[...] = squares
                q1[...] = to_row(sqs[self.other, :])
                self.copies.append(send(q1, p1, side, 0, sibling))

        def cross(self):
            c = self.which
            for copy in self.copies:
                copy.wait()
            pair = tot[c][self.mine, :] + r1[c][...].astype(jnp.float32)
            s2[c][...] = pair.astype(jnp.bfloat16)
            spots = [self.parity * hops + k for k in range(hops)]
            self.copies = [
                send(s2[c], r2[c].at[spot], main, self.base + 2 + spot, peer)
                for spot, peer in zip(spots, partners)
            ]
            tot[c][self.mine, :] = pair
            if self.squares:
                self.row = to_row(sqs[self.mine, :]) + p1[...]
                q2[...] = self.row
                self.copies += [
                    send(q2, p2.at[spot], side, 2 + spot, peer)
                    for spot, peer in zip(spots, partners)
                ]

        def back(self):
            c = self.which
            for copy in self.copies:
                copy.wait()
            total = tot[c][self.mine, :]
            for k in range(hops):
                total = total + r2[c][self.parity * hops + k].astype(jnp.float32)
            s3[c][...] = total.astype(jnp.bfloat16)
            self.copies = [send(s3[c], r3[c], main, self.base + 1, sibling)]
            tot[c][self.mine, :] = total
            if self.squares:
                row = self.row
                for k in range(hops):
                    row = row + p2[self.parity * hops + k]
                q3[...] = row
                self.copies.append(send(q3, p3, side, 1, sibling))
                sqs[self.mine, :] = to_column(row)

        def end(self):
            c = self.which
            for copy in self.copies:
                copy.wait()
            tot[c][self.other, :] = r3[c][...].astype(jnp.float32)
            if self.squares:
                sqs[self.other, :] = to_column(p3[...])
            return tot[c][...]

    forth, own_act, low_act, cross_weight, low_input, first_slope, first_gram = [
        Channel(k) for k in range(7)
    ]

    def update(w, m, layer, grad, last):
        moment = moment_decay * m[layer] + grad
        m[layer] = moment
        if last and levels:
            return
        w[layer] = (w[layer].astype(jnp.float32) - learn_rate * moment).astype(jnp.bfloat16)

    def update_up(layer, last):
        update(wu, mu, layer, dot_nn(act[layer].T, gr[...].astype(jnp.bfloat16)) * r_scale, last)

    def update_down(layer, rows_t, last):
        update(wd, md, layer, dot_nn(rows_t, low[layer]) * d_scale, last)

    def activate(layer, preact):
        activation = (preact * jax.nn.sigmoid(preact)).astype(jnp.bfloat16)
        pre[layer] = preact
        act[layer] = activation
        return activation

    def low_grads(layer, grad_act):
        preact = pre[layer]
        sig = jax.nn.sigmoid(preact)
        grad_pre = grad_act * (sig * (1.0 + preact * (1.0 - sig)))
        low[layer] = (grad_pre * inv[layer]).astype(jnp.bfloat16)
        return jnp.sum(grad_pre * preact, axis=1, keepdims=True)

    down, up = (wdl, got_wd, res_wd), (wul, got_wu, res_wu)
    mdown, mup = (mdl, got_md, res_md), (mul, got_mu, res_mu)
    layers = list(reversed(range(wd.shape[0])))
    chunks = []
    for pairs in ((up, down), (mup, mdown)):
        for layer in layers:
            for pair, wide in zip(pairs, (False, True)):
                for form, base, size in cuts(pair[0].shape[1], wide):
                    chunks.append((pair, layer, form, base, size))
    first = len(chunks) // 2
    part = first // 4
    sent = []

    class Piece:
        def __init__(self, index):
            (self.acc, self.got, self.res), self.layer, self.form, self.base, self.size = chunks[index]
            self.index = index
            self.stages = 7 if self.form == "fold" else 9

        def rows(self, ref, start, size, slot=0):
            first_row = self.base + (slot - 1 if slot else 0) * self.acc.shape[1]
            start = start + first_row
            if not isinstance(start, int):
                start = pl.multiple_of(start, 16)
            return ref.at[self.layer, pl.ds(start, size)]

        def copy(self, kind, src, dst, peer):
            index = self.index * KINDS + kind
            return pltpu.make_async_remote_copy(
                src_ref=src, dst_ref=dst,
                send_sem=row_send.at[index], recv_sem=row_recv.at[index],
                device_id={"row": peer}, device_id_type=MESH,
            )

        def sum_out(self, kind, start, size, slot, landing, peer, when=None):
            def go(finish=False):
                made = self.copy(
                    kind, self.rows(self.acc, start, size), self.rows(self.got, landing, size, slot), peer
                )
                made.wait_send() if finish else made.start()

            go()
            sent.append((when, functools.partial(go, True)))

        def mean_out(self, kind, start, size, peer, when=None):
            def go(finish=False):
                where = self.rows(self.res, start, size)
                made = self.copy(kind, where, where, peer)
                made.wait_send() if finish else made.start()

            go()
            sent.append((when, functools.partial(go, True)))

        def landed(self, kind, start, size, slot=0):
            ref = self.rows(self.got, start, size, slot) if slot else self.rows(self.res, start, size)
            self.copy(kind, ref, ref, facing).wait_recv()

        def add(self, start, size, slot, landing):
            mine = self.rows(self.acc, start, size)
            came = self.rows(self.got, landing, size, slot)
            total = mine[...].astype(jnp.float32) + came[...].astype(jnp.float32)
            mine[...] = total.astype(jnp.bfloat16)

        def settle(self, start, size, slot, landing):
            mine = self.rows(self.acc, start, size)
            came = self.rows(self.got, landing, size, slot)
            total = mine[...].astype(jnp.float32) + came[...].astype(jnp.float32)
            self.rows(self.res, start, size)[...] = (total * (1.0 / replicas)).astype(jnp.bfloat16)

        def run(self, stage):
            (self.fold if self.form == "fold" else self.line)(stage)

        def fold(self, stage):
            half_size, quarter = self.size // 2, self.size // 4
            keep, away = side_of * half_size, (1 - side_of) * half_size
            outer = (line == 0) | (line == LINES - 1)
            inner = jnp.logical_not(outer)
            upper = lax.rem(line // 2, 2)
            inward = spot + 2 - 4 * upper
            outward = spot - 2 + 4 * upper
            across = spot + 2 - 4 * upper
            own = keep + upper * quarter
            far = keep + (1 - upper) * quarter
            if stage == 0:
                self.sum_out(0, away, half_size, 1, 0, facing)
            elif stage == 1:
                self.landed(0, 0, half_size, 1)
                self.add(keep, half_size, 1, 0)

                @pl.when(outer)
                def _():
                    self.sum_out(1, keep, half_size, 2, 0, inward, outer)
            elif stage == 2:

                @pl.when(inner)
                def _():
                    self.landed(1, 0, half_size, 2)
                    self.add(keep, half_size, 2, 0)
                    self.sum_out(2, far, quarter, 3, 0, across, inner)
            elif stage == 3:

                @pl.when(inner)
                def _():
                    self.landed(2, 0, quarter, 3)
                    self.settle(own, quarter, 3, 0)
                    self.mean_out(3, own, quarter, across, inner)
            elif stage == 4:

                @pl.when(inner)
                def _():
                    self.landed(3, far, quarter)
                    self.mean_out(4, keep, half_size, outward, inner)
                    self.mean_out(5, keep, half_size, facing, inner)
            elif stage == 5:

                @pl.when(outer)
                def _():
                    self.landed(4, keep, half_size)
                    self.mean_out(5, keep, half_size, facing, outer)
            else:
                self.landed(5, away, half_size)

        def line(self, stage):
            piece = self.size // LINES
            fine = piece // 2
            end = LINES - 1
            if stage <= end:
                for at, step_to, kind, slot in ((stage, 1, 0, 1), (end - stage, -1, 1, 2)):
                    ahead = (at + 1) * piece if step_to > 0 else 0
                    count = (end - at) * piece if step_to > 0 else at * piece
                    came = (LINES - at) * piece if step_to > 0 else (at + 1) * piece
                    opened = at * piece if step_to > 0 else 0
                    here = line == at

                    @pl.when(here)
                    def _(ahead=ahead, count=count, came=came, opened=opened, kind=kind, slot=slot, here=here, peer=after if step_to > 0 else before):
                        if stage:
                            self.landed(kind, opened, came, slot)
                        if count:
                            if stage:
                                self.add(ahead, count, slot, ahead)
                            self.sum_out(kind, ahead, count, slot, ahead, peer, here)
            if stage == end:
                own = line * piece

                @pl.when(line > 0)
                def _():
                    self.add(own, piece, 1, own)

                @pl.when(line < end)
                def _():
                    self.add(own, piece, 2, own)

                self.sum_out(2, own + (1 - side_of) * fine, fine, 3, 0, facing)
            elif stage == end + 1:
                own = line * piece + side_of * fine
                self.landed(2, 0, fine, 3)
                self.settle(own, fine, 3, 0)
                self.mean_out(3, own, fine, facing)
            elif stage > end + 1:
                hop = stage - end - 2
                if hop == 0:
                    self.landed(3, line * piece + (1 - side_of) * fine, fine)
                for at, step_to, kind in ((hop, 1, 4), (end - hop, -1, 5)):
                    here = line == at
                    came = hop * piece
                    opened = 0 if step_to > 0 else (at + 1) * piece
                    begun = 0 if step_to > 0 else at * piece

                    @pl.when(here)
                    def _(came=came, opened=opened, begun=begun, kind=kind, here=here, peer=after if step_to > 0 else before):
                        if hop:
                            self.landed(kind, opened, came)
                        if hop < end:
                            self.mean_out(kind, begun, came + piece, peer, here)

    pieces = [Piece(k) for k in range(len(chunks))] if levels else []
    done = {k: 0 for k in range(len(chunks))}
    plan = sorted(
        (0.25 * (k % first) + (2.0 if k >= first else 0.0) + stage, k, stage)
        for k, piece in enumerate(pieces)
        for stage in range(1, piece.stages)
    )

    def start(picked):
        for k in picked if levels else []:
            pieces[k].run(0)

    def advance(count=None, below=None):
        taken = 0
        for entry in list(plan):
            if taken == count:
                break
            if below is not None and entry[1] >= below:
                continue
            pieces[entry[1]].run(entry[2])
            plan.remove(entry)
            taken += 1

    def step(parity, last, deferred):
        if last:
            wul[...] = wu[...]
            wdl[1] = wd[1]
            start(range(first - part))
        activation = activate(0, proj[...] * inv[0])
        lifted = dot_nn(activation, wu[0]) * r_scale
        x1[...] = (x0_ref[...].astype(jnp.float32) + lifted).astype(jnp.bfloat16)
        wide = x1[...].astype(jnp.float32)
        squares = jnp.sum(wide * wide, axis=1, keepdims=True)
        forth.begin(parity, dot_nn(x1[...], wd[1]) * d_scale, squares)
        cross_weight.begin(parity, dot_nn(wu[0], wd[1]) * (r_scale * d_scale))
        forth.cross()
        low_input.begin(parity, dot_nt(x1[...], wu[0]) * r_scale)
        cross_weight.cross()
        low_input.cross()
        x1t[...] = x1[...].T
        deferred()
        if last:
            wdl[0] = wd[0]
            start(range(first - part, first))
            advance(4, first)
        forth.back()
        forth.end()
        inv[1] = lax.rsqrt(sqs[...] / full + norm_eps)
        activation = activate(1, tot[0][...] * inv[1])
        lifted = dot_nn(activation, wu[1]) * r_scale
        outcome = (x1[...].astype(jnp.float32) + lifted).astype(jnp.bfloat16)
        gr[...] = outcome.astype(jnp.float32) - tg_ref[...].astype(jnp.float32)
        grad_low = gr[...].astype(jnp.bfloat16)
        own_act.begin(parity, dot_nt(grad_low, wu[1]) * r_scale)
        low_act.begin(parity, dot_nt(grad_low, wu[0]) * r_scale)
        own_act.cross()
        low_act.cross()
        update_up(1, last)
        cross_weight.back()
        low_input.back()
        if last:
            advance(6, first)
        own_act.back()
        row_dot = low_grads(1, own_act.end())
        coefficient = row_dot * inv[1] * inv[1] / full
        through = dot_nt(low[1], wd[1]) * d_scale
        gr[...] = gr[...] + through - coefficient * x1[...].astype(jnp.float32)
        low_act.back()
        update_up(0, last)
        update_down(1, x1t[...], last)
        weight = cross_weight.end().astype(jnp.bfloat16)
        grad_act = dot_nt(low[1], weight) - coefficient * low_input.end()
        low_grads(0, low_act.end() + grad_act)
        if last:
            return
        slope[...] = moment_decay * slope[...] + dot_nn(gram[...], low[0]) * (d_scale * d_scale)
        proj[...] = proj[...] - learn_rate * slope[...]

    def late_down(last=False):
        update_down(0, xt[...], last)

    def carried():
        first_slope.back()
        first_gram.back()
        slope[...] = first_slope.end()
        gram[...] = first_gram.end().astype(jnp.bfloat16)

    def middle(index, carry):
        def deferred():
            pl.when(index == 0)(carried)
            pl.when(index > 0)(late_down)

        step(lax.rem(index, 2), False, deferred)
        return carry

    loads[0].wait()
    xt[...] = x0_ref[...].T
    wide_input = x0_ref[...].astype(jnp.float32)
    squares = jnp.sum(wide_input * wide_input, axis=1, keepdims=True)
    loads[1].wait()
    forth.begin(1, dot_nn(x0_ref[...], wd[0]) * d_scale, squares)
    loads[2].wait()
    first_slope.begin(1, dot_nn(x0_ref[...], md[0].astype(jnp.bfloat16)) * d_scale)
    first_gram.begin(1, dot_nn(x0_ref[...], xt[...]))
    forth.cross()
    first_slope.cross()
    first_gram.cross()
    for load in loads[3:]:
        load.wait()
    forth.back()
    proj[...] = forth.end()
    inv[0] = lax.rsqrt(sqs[...] / full + norm_eps)
    lax.fori_loop(0, STEPS - 1, middle, 0)
    step((STEPS - 1) % 2, True, late_down)
    if levels:
        mul[...] = mu[...].astype(jnp.bfloat16)
        mdl[1] = md[1].astype(jnp.bfloat16)
        start(range(first, len(chunks) - part))
    late_down(True)
    mdl[0] = md[0].astype(jnp.bfloat16)
    if not levels:
        mul[...] = mu[...].astype(jnp.bfloat16)
        mdl[1] = md[1].astype(jnp.bfloat16)
    outs = ((wd_out, res_wd, wd), (wu_out, res_wu, wu), (md_out, res_md, mdl), (mu_out, res_mu, mul))
    if not levels:
        stores = [pltpu.make_async_copy(kept, out, store_sem.at[k]) for k, (out, _, kept) in enumerate(outs)]
        for store in stores:
            store.start()
        for store in stores:
            store.wait()
        return
    start(range(len(chunks) - part, len(chunks)))
    advance()
    stores = []
    for piece in pieces:
        for out, res, _ in outs:
            if res is piece.res:
                stores.append(pltpu.make_async_copy(
                    piece.rows(res, 0, piece.size), piece.rows(out, 0, piece.size), store_sem.at[piece.index]
                ))
                stores[-1].start()
    for when, finish in sent:
        if when is None:
            finish()
        else:
            pl.when(when)(finish)
    for store in stores:
        store.wait()


def finish_kernel(wd_ref, wu_ref, md_ref, mu_ref, wd_out, wu_out, md_out, mu_out):
    for w_ref, m_ref, w_out, m_out in ((wd_ref, md_ref, wd_out, md_out), (wu_ref, mu_ref, wu_out, mu_out)):
        moments = m_ref[...].astype(jnp.float32)
        moved = w_ref[...].astype(jnp.float32) - learn_rate * moments
        w_out[...] = moved.astype(jnp.bfloat16)
        m_out[...] = moments


def finish(means):
    layers = means[0].shape[0]
    parts = 2
    specs = [
        pl.BlockSpec((1, mean.shape[1] // parts, mean.shape[2]), lambda i: (i // parts, i % parts, 0))
        for mean in means
    ]
    kinds = [jnp.bfloat16, jnp.bfloat16, jnp.float32, jnp.float32]
    return pl.pallas_call(
        finish_kernel,
        grid=(layers * parts,),
        out_shape=[jax.ShapeDtypeStruct(mean.shape, kind) for mean, kind in zip(means, kinds)],
        in_specs=specs,
        out_specs=specs,
    )(*means)


def fused(shards, replicas, hidden, target, w_down, w_up, m_down, m_up):
    tok, width = hidden.shape
    layers, _, rank = w_down.shape
    half = tok // 2
    hops = shards // 2 - 1
    bf, f32 = jnp.bfloat16, jnp.float32
    hbm = pl.BlockSpec(memory_space=pl.ANY)
    channels = 7
    sems = channels * (2 + 2 * hops)
    rows = [tok, tok, tok, rank, tok, tok, tok]
    halves = [pltpu.VMEM((count // 2, rank), bf) for count in rows]
    crossed = [pltpu.VMEM((2 * hops, count // 2, rank), bf) for count in rows]
    totals = [pltpu.VMEM((count, rank), f32) for count in rows]
    row_sems = 8 * layers * KINDS
    tripled = [(layers, 3 * count, other) for count, other in (w_down.shape[1:], w_up.shape[1:])] * 2
    return pl.pallas_call(
        functools.partial(fused_kernel, shards, replicas),
        out_shape=[
            jax.ShapeDtypeStruct(w_down.shape, bf),
            jax.ShapeDtypeStruct(w_up.shape, bf),
            jax.ShapeDtypeStruct(m_down.shape, bf),
            jax.ShapeDtypeStruct(m_up.shape, bf),
        ],
        in_specs=[hbm] * 6,
        out_specs=[hbm] * 4,
        scratch_shapes=[
            pltpu.VMEM(hidden.shape, bf),
            pltpu.VMEM(target.shape, bf),
            pltpu.VMEM(w_down.shape, bf),
            pltpu.VMEM(w_up.shape, bf),
            pltpu.VMEM(m_down.shape, f32),
            pltpu.VMEM(m_up.shape, f32),
            pltpu.SemaphoreType.DMA((6,)),
            pltpu.SemaphoreType.DMA((8 * layers,)),
            pltpu.VMEM(w_down.shape, bf),
            pltpu.VMEM(w_up.shape, bf),
            pltpu.VMEM(m_down.shape, bf),
            pltpu.VMEM(m_up.shape, bf),
            pltpu.VMEM(w_down.shape, bf),
            pltpu.VMEM(w_up.shape, bf),
            pltpu.VMEM(m_down.shape, bf),
            pltpu.VMEM(m_up.shape, bf),
            pltpu.VMEM(tripled[0], bf),
            pltpu.VMEM(tripled[1], bf),
            pltpu.VMEM(tripled[2], bf),
            pltpu.VMEM(tripled[3], bf),
            pltpu.SemaphoreType.DMA((row_sems,)),
            pltpu.SemaphoreType.DMA((row_sems,)),
            pltpu.VMEM((tok, width), bf),
            pltpu.VMEM((width, tok), bf),
            pltpu.VMEM((width, tok), bf),
            pltpu.VMEM((tok, width), f32),
            pltpu.VMEM((layers, tok, rank), f32),
            pltpu.VMEM((layers, tok, rank), bf),
            pltpu.VMEM((layers, tok, 1), f32),
            pltpu.VMEM((layers, tok, rank), bf),
            pltpu.VMEM((tok, rank), f32),
            pltpu.VMEM((tok, rank), f32),
            pltpu.VMEM((tok, tok), bf),
            pltpu.VMEM((tok, 1), f32),
            halves,
            halves,
            halves,
            crossed,
            halves,
            halves,
            totals,
            pltpu.VMEM((8, half), f32),
            pltpu.VMEM((8, half), f32),
            pltpu.VMEM((8, half), f32),
            pltpu.VMEM((2 * hops, 8, half), f32),
            pltpu.VMEM((8, half), f32),
            pltpu.VMEM((8, half), f32),
            pltpu.SemaphoreType.DMA((sems,)),
            pltpu.SemaphoreType.DMA((sems,)),
            pltpu.SemaphoreType.DMA((2 + 2 * hops,)),
            pltpu.SemaphoreType.DMA((2 + 2 * hops,)),
        ],
        compiler_params=pltpu.CompilerParams(
            collective_id=0, has_side_effects=True, vmem_limit_bytes=60 * 1024 * 1024
        ),
    )(hidden, target, w_down, w_up, m_down, m_up)


def body(shards, replicas, hidden, target, w_down, w_up, m_down, m_up):
    means = fused(
        shards, replicas, hidden[0], target[0], w_down[0], w_up[0], m_down[0], m_up[0]
    )
    if on_grid(replicas, hidden.shape[2], w_down.shape[3]):
        return tuple(finish(means))
    totals = lax.psum(tuple(means), "row")
    means = [total.astype(jnp.float32) / replicas for total in totals]
    return (
        means[0].astype(jnp.bfloat16),
        means[1].astype(jnp.bfloat16),
        means[2].astype(jnp.float32),
        means[3].astype(jnp.float32),
    )


def solution(mesh):
    placed = (
        P("row", None, "ta"),
        P("row", None, "ta"),
        P("row", None, "ta", None),
        P("row", None, None, "ta"),
        P("row", None, "ta", None),
        P("row", None, None, "ta"),
    )
    return jax.shard_map(
        functools.partial(body, mesh.shape["ta"], mesh.shape["row"]),
        mesh=mesh,
        in_specs=placed,
        out_specs=(
            P(None, "ta", None),
            P(None, None, "ta"),
            P(None, "ta", None),
            P(None, None, "ta"),
        ),
        check_vma=False,
    )
```

```python
import functools

import jax
import jax.numpy as jnp
from jax import lax
from jax.experimental import pallas as pl
from jax.experimental.pallas import tpu as pltpu
from jax.sharding import PartitionSpec as P

MESH = pl.DeviceIdType.MESH
STEPS = 4
norm_eps = 1e-06
learn_rate = 0.02
moment_decay = 0.9


def dot_nn(a, b):
    return jnp.dot(a, b, preferred_element_type=jnp.float32)


def dot_nt(a, b):
    return lax.dot_general(a, b, (((1,), (1,)), ((), ())), preferred_element_type=jnp.float32)


LINES = 4
FOLD_PARTS, LINE_PARTS = 5, 2
KINDS = 6
ORDER = [
    (7, 1), (0, 1), (2, 1), (0, 2), (12, 1), (1, 1), (3, 1), (4, 1), (1, 2), (3, 2), (0, 3), (17, 1), (2, 2),
    (2, 3), (4, 2), (0, 4), (5, 1), (5, 2), (12, 2), (10, 1), (6, 1), (8, 1), (9, 1), (0, 5), (1, 3), (7, 2),
    (10, 2), (3, 3), (17, 2), (5, 3), (4, 3), (11, 1), (6, 2), (17, 3), (7, 3), (1, 4), (10, 3), (15, 1),
    (12, 3), (5, 4), (4, 4), (9, 2), (13, 1), (11, 2), (6, 3), (8, 2), (1, 5), (19, 1), (2, 4), (5, 5),
    (10, 4), (17, 4), (9, 3), (3, 4), (11, 3), (14, 1), (7, 4), (13, 2), (6, 4), (4, 5), (19, 2), (8, 3),
    (14, 2), (15, 2), (11, 4), (13, 3), (19, 3), (9, 4), (8, 4), (14, 3), (2, 5), (15, 3), (13, 4), (18, 1),
    (18, 2), (16, 1), (12, 4), (10, 5), (3, 5), (11, 5), (5, 6), (19, 4), (16, 2), (7, 5), (17, 5), (9, 5),
    (8, 5), (2, 6), (14, 4), (15, 4), (17, 6), (16, 3), (18, 3), (7, 6), (2, 7), (6, 5), (1, 6), (13, 5),
    (14, 5), (16, 4), (18, 4), (3, 6), (8, 6), (12, 5), (19, 5), (15, 5), (11, 6), (17, 7), (12, 6), (16, 5),
    (6, 6), (7, 7), (4, 6), (13, 6), (15, 6), (19, 6), (10, 6), (14, 6), (18, 5), (12, 7), (9, 6), (0, 6),
    (7, 8), (18, 6), (16, 6), (17, 8), (2, 8), (12, 8),
]


def on_grid(replicas, width, rank):
    return replicas == 2 * LINES and width % 128 == 0 and rank % 128 == 0 and width >= 512


def cuts(length, wide):
    if not wide:
        return [("fold", k * (length // 2), length // 2) for k in range(2)]
    line = length * LINE_PARTS // (FOLD_PARTS + LINE_PARTS) // 128 * 128
    size = (length - line) // 2
    return [("line", 0, line), ("fold", line, size), ("fold", line + size, size)]


def fused_kernel(
    shards, replicas,
    x0_in, tg_in, wd_in, wu_in, md_in, mu_in,
    wd_out, wu_out, md_out, mu_out,
    x0_ref, tg_ref, wd, wu, md, mu, load_sem, store_sem, wdl, wul, mdl, mul, res_wd, res_wu, res_md, res_mu,
    got_wd, got_wu, got_md, got_mu, row_send, row_recv,
    x1, x1t, xt, gr, pre, bend, act, inv, low, proj, slope, gram, sqs,
    s1, r1, s2, r2, s3, r3, tot, q1, p1, q2, p2,
    main_send, main_recv, side_send, side_recv,
):
    tok, width = x0_ref.shape
    rank = wd.shape[2]
    loads = [
        pltpu.make_async_copy(source, target, load_sem.at[k])
        for k, (source, target) in enumerate((
            (x0_in, x0_ref), (wd_in, wd), (md_in, md), (wu_in, wu), (tg_in, tg_ref), (mu_in, mu),
        ))
    ]
    for load in loads:
        load.start()
    full = width * shards
    chips = shards // 2
    me = lax.axis_index("ta")
    core = lax.rem(me, 2)
    sibling = me + 1 - 2 * core
    partners = [lax.rem(me + 2 * k, shards) for k in range(1, chips)]
    hops = chips - 1
    d_scale = full ** (-0.5)
    r_scale = rank ** (-0.5)

    barrier = pltpu.get_barrier_semaphore()
    for peer in [sibling] + partners:
        pl.semaphore_signal(barrier, inc=1, device_id={"ta": peer}, device_id_type=MESH)
    levels = on_grid(replicas, width, rank)
    spot = lax.axis_index("row")
    line, side_of = spot // 2, lax.rem(spot, 2)
    facing = spot + 1 - 2 * side_of
    after, before = lax.rem(spot + 2, replicas), lax.rem(spot + replicas - 2, replicas)
    greeted = [facing, after, before] if levels else []
    for peer in greeted:
        pl.semaphore_signal(barrier, inc=1, device_id={"row": peer}, device_id_type=MESH)
    pl.semaphore_wait(barrier, chips + len(greeted))

    def send(src, dst, sems, index, peer):
        copy = pltpu.make_async_remote_copy(
            src_ref=src, dst_ref=dst,
            send_sem=sems[0].at[index], recv_sem=sems[1].at[index],
            device_id={"ta": peer}, device_id_type=MESH,
        )
        copy.start()
        return copy

    main = (main_send, main_recv)
    side = (side_send, side_recv)
    per_channel = 2 + 2 * hops

    def to_column(row):
        return jnp.broadcast_to(row[0:1, :], (tok, tok)).T[:, 0:1]

    def row_squares(rows):
        wide = rows.astype(jnp.float32)
        return dot_nt(jnp.ones((8, width), jnp.bfloat16), (wide * wide).astype(jnp.bfloat16))

    class Channel:
        def __init__(self, which):
            self.which = which
            self.size = tot[which].shape[0] // 2
            size = self.size
            self.mine = pl.ds(pl.multiple_of(core * size, size), size)
            self.other = pl.ds(pl.multiple_of((1 - core) * size, size), size)
            self.base = which * per_channel

        def begin(self, parity, value, squares=None):
            c = self.which
            self.parity = parity
            self.squares = squares is not None
            tot[c][...] = value
            s1[c][...] = tot[c][self.other, :].astype(jnp.bfloat16)
            self.copies = [send(s1[c], r1[c], main, self.base, sibling)]
            if self.squares:
                q1[...] = squares
                self.copies.append(send(q1, p1, side, 0, sibling))

        def cross(self):
            c = self.which
            for copy in self.copies:
                copy.wait()
            pair = tot[c][self.mine, :] + r1[c][...].astype(jnp.float32)
            s2[c][...] = pair.astype(jnp.bfloat16)
            spots = [self.parity * hops + k for k in range(hops)]
            self.copies = [
                send(s2[c], r2[c].at[spot], main, self.base + 2 + spot, peer)
                for spot, peer in zip(spots, partners)
            ]
            tot[c][self.mine, :] = pair
            if self.squares:
                q2[...] = q1[...] + p1[...]
                self.copies += [
                    send(q2, p2.at[spot], side, 2 + spot, peer)
                    for spot, peer in zip(spots, partners)
                ]

        def back(self):
            c = self.which
            for copy in self.copies:
                copy.wait()
            total = tot[c][self.mine, :]
            for k in range(hops):
                total = total + r2[c][self.parity * hops + k].astype(jnp.float32)
            s3[c][...] = total.astype(jnp.bfloat16)
            self.copies = [send(s3[c], r3[c], main, self.base + 1, sibling)]
            tot[c][self.mine, :] = total
            if self.squares:
                row = q2[...]
                for k in range(hops):
                    row = row + p2[self.parity * hops + k]
                sqs[...] = to_column(row)

        def end(self):
            c = self.which
            for copy in self.copies:
                copy.wait()
            tot[c][self.other, :] = r3[c][...].astype(jnp.float32)
            return tot[c][...]

    forth, own_act, low_act, cross_weight, low_input, first_slope, first_gram = [
        Channel(k) for k in range(7)
    ]

    def update(w, m, layer, grad, last):
        moment = moment_decay * m[layer] + grad
        m[layer] = moment
        if last and levels:
            return
        w[layer] = (w[layer].astype(jnp.float32) - learn_rate * moment).astype(jnp.bfloat16)

    def update_up(layer, last):
        update(wu, mu, layer, dot_nn(act[layer].T, gr[...].astype(jnp.bfloat16)) * r_scale, last)

    def update_down(layer, rows_t, last):
        update(wd, md, layer, dot_nn(rows_t, low[layer]) * d_scale, last)

    def activate(layer, preact):
        activation = (preact * jax.nn.sigmoid(preact)).astype(jnp.bfloat16)
        pre[layer] = preact
        act[layer] = activation
        return activation

    def ready_slope(layer):
        preact = pre[layer]
        sig = jax.nn.sigmoid(preact)
        steep = sig * (1.0 + preact * (1.0 - sig))
        bend[layer] = steep * inv[layer]
        pre[layer] = steep * preact

    def low_grads(layer, grad_act):
        low[layer] = (grad_act * bend[layer]).astype(jnp.bfloat16)

    down, up = (wdl, got_wd, res_wd), (wul, got_wu, res_wu)
    mdown, mup = (mdl, got_md, res_md), (mul, got_mu, res_mu)
    layers = list(reversed(range(wd.shape[0])))
    chunks = []
    for pairs in ((up, down), (mup, mdown)):
        for layer in layers:
            for pair, wide in zip(pairs, (False, True)):
                for form, base, size in cuts(pair[0].shape[1], wide):
                    chunks.append((pair, layer, form, base, size))
    first = len(chunks) // 2
    part = len(cuts(width, True))
    up_part = len(cuts(rank, False))
    sent = []

    class Piece:
        def __init__(self, index):
            (self.acc, self.got, self.res), self.layer, self.form, self.base, self.size = chunks[index]
            self.index = index
            self.stages = 7 if self.form == "fold" else 9

        def rows(self, ref, start, size, slot=0):
            first_row = self.base + (slot - 1 if slot else 0) * self.acc.shape[1]
            start = start + first_row
            if not isinstance(start, int):
                start = pl.multiple_of(start, 16)
            return ref.at[self.layer, pl.ds(start, size)]

        def copy(self, kind, src, dst, peer):
            index = self.index * KINDS + kind
            return pltpu.make_async_remote_copy(
                src_ref=src, dst_ref=dst,
                send_sem=row_send.at[index], recv_sem=row_recv.at[index],
                device_id={"row": peer}, device_id_type=MESH,
            )

        def sum_out(self, kind, start, size, slot, landing, peer, when=None):
            def go(finish=False):
                made = self.copy(
                    kind, self.rows(self.acc, start, size), self.rows(self.got, landing, size, slot), peer
                )
                made.wait_send() if finish else made.start()

            go()
            sent.append((when, functools.partial(go, True)))

        def mean_out(self, kind, start, size, peer, when=None):
            def go(finish=False):
                where = self.rows(self.res, start, size)
                made = self.copy(kind, where, where, peer)
                made.wait_send() if finish else made.start()

            go()
            sent.append((when, functools.partial(go, True)))

        def landed(self, kind, start, size, slot=0):
            ref = self.rows(self.got, start, size, slot) if slot else self.rows(self.res, start, size)
            self.copy(kind, ref, ref, facing).wait_recv()

        def add(self, start, size, slot, landing):
            mine = self.rows(self.acc, start, size)
            came = self.rows(self.got, landing, size, slot)
            total = mine[...].astype(jnp.float32) + came[...].astype(jnp.float32)
            mine[...] = total.astype(jnp.bfloat16)

        def settle(self, start, size, slot, landing):
            mine = self.rows(self.acc, start, size)
            came = self.rows(self.got, landing, size, slot)
            total = mine[...].astype(jnp.float32) + came[...].astype(jnp.float32)
            self.rows(self.res, start, size)[...] = (total * (1.0 / replicas)).astype(jnp.bfloat16)

        def run(self, stage):
            (self.fold if self.form == "fold" else self.line)(stage)

        def fold(self, stage):
            half_size, quarter = self.size // 2, self.size // 4
            keep, away = side_of * half_size, (1 - side_of) * half_size
            outer = (line == 0) | (line == LINES - 1)
            inner = jnp.logical_not(outer)
            upper = lax.rem(line // 2, 2)
            inward = spot + 2 - 4 * upper
            outward = spot - 2 + 4 * upper
            across = spot + 2 - 4 * upper
            own = keep + upper * quarter
            far = keep + (1 - upper) * quarter
            if stage == 0:
                self.sum_out(0, away, half_size, 1, 0, facing)
            elif stage == 1:
                self.landed(0, 0, half_size, 1)
                self.add(keep, half_size, 1, 0)

                @pl.when(outer)
                def _():
                    self.sum_out(1, keep, half_size, 2, 0, inward, outer)
            elif stage == 2:

                @pl.when(inner)
                def _():
                    self.landed(1, 0, half_size, 2)
                    self.add(keep, half_size, 2, 0)
                    self.sum_out(2, far, quarter, 3, 0, across, inner)
            elif stage == 3:

                @pl.when(inner)
                def _():
                    self.landed(2, 0, quarter, 3)
                    self.settle(own, quarter, 3, 0)
                    self.mean_out(3, own, quarter, across, inner)
            elif stage == 4:

                @pl.when(inner)
                def _():
                    self.landed(3, far, quarter)
                    self.mean_out(4, keep, half_size, outward, inner)
                    self.mean_out(5, keep, half_size, facing, inner)
            elif stage == 5:

                @pl.when(outer)
                def _():
                    self.landed(4, keep, half_size)
                    self.mean_out(5, keep, half_size, facing, outer)
            else:
                self.landed(5, away, half_size)

        def line(self, stage):
            piece = self.size // LINES
            fine = piece // 2
            end = LINES - 1
            if stage <= end:
                for at, step_to, kind, slot in ((stage, 1, 0, 1), (end - stage, -1, 1, 2)):
                    ahead = (at + 1) * piece if step_to > 0 else 0
                    count = (end - at) * piece if step_to > 0 else at * piece
                    came = (LINES - at) * piece if step_to > 0 else (at + 1) * piece
                    opened = at * piece if step_to > 0 else 0
                    here = line == at

                    @pl.when(here)
                    def _(ahead=ahead, count=count, came=came, opened=opened, kind=kind, slot=slot, here=here, peer=after if step_to > 0 else before):
                        if stage:
                            self.landed(kind, opened, came, slot)
                        if count:
                            if stage:
                                self.add(ahead, count, slot, ahead)
                            self.sum_out(kind, ahead, count, slot, ahead, peer, here)
            if stage == end:
                own = line * piece

                @pl.when(line > 0)
                def _():
                    self.add(own, piece, 1, own)

                @pl.when(line < end)
                def _():
                    self.add(own, piece, 2, own)

                self.sum_out(2, own + (1 - side_of) * fine, fine, 3, 0, facing)
            elif stage == end + 1:
                own = line * piece + side_of * fine
                self.landed(2, 0, fine, 3)
                self.settle(own, fine, 3, 0)
                self.mean_out(3, own, fine, facing)
            elif stage > end + 1:
                hop = stage - end - 2
                if hop == 0:
                    self.landed(3, line * piece + (1 - side_of) * fine, fine)
                for at, step_to, kind in ((hop, 1, 4), (end - hop, -1, 5)):
                    here = line == at
                    came = hop * piece
                    opened = 0 if step_to > 0 else (at + 1) * piece
                    begun = 0 if step_to > 0 else at * piece

                    @pl.when(here)
                    def _(came=came, opened=opened, begun=begun, kind=kind, here=here, peer=after if step_to > 0 else before):
                        if hop:
                            self.landed(kind, opened, came)
                        if hop < end:
                            self.mean_out(kind, begun, came + piece, peer, here)

    pieces = [Piece(k) for k in range(len(chunks))] if levels else []
    done = {k: 0 for k in range(len(chunks))}
    plan = list(ORDER) if levels else []

    def start(picked):
        for k in picked if levels else []:
            pieces[k].run(0)

    def advance(count=None, below=None):
        taken = 0
        for entry in list(plan):
            if taken == count:
                break
            if below is not None and entry[0] >= below:
                continue
            pieces[entry[0]].run(entry[1])
            plan.remove(entry)
            taken += 1

    def step(parity, last, deferred):
        if last:
            wul[...] = wu[...]
            wdl[1] = wd[1]
            start(range(first - part))
        activation = activate(0, proj[...] * inv[0])
        lifted = dot_nn(activation, wu[0]) * r_scale
        x1[...] = (x0_ref[...].astype(jnp.float32) + lifted).astype(jnp.bfloat16)
        forth.begin(parity, dot_nn(x1[...], wd[1]) * d_scale, row_squares(x1[...]))
        cross_weight.begin(parity, dot_nn(wu[0], wd[1]) * (r_scale * d_scale))
        forth.cross()
        low_input.begin(parity, dot_nt(x1[...], wu[0]) * r_scale)
        cross_weight.cross()
        low_input.cross()
        x1t[...] = x1[...].T
        ready_slope(0)
        deferred()
        if last:
            wdl[0] = wd[0]
            start(range(first - part, first))
            advance(3, first)
        forth.back()
        forth.end()
        inv[1] = lax.rsqrt(sqs[...] / full + norm_eps)
        activation = activate(1, tot[0][...] * inv[1])
        lifted = dot_nn(activation, wu[1]) * r_scale
        outcome = (x1[...].astype(jnp.float32) + lifted).astype(jnp.bfloat16)
        gr[...] = outcome.astype(jnp.float32) - tg_ref[...].astype(jnp.float32)
        grad_low = gr[...].astype(jnp.bfloat16)
        own_act.begin(parity, dot_nt(grad_low, wu[1]) * r_scale)
        low_act.begin(parity, dot_nt(grad_low, wu[0]) * r_scale)
        own_act.cross()
        low_act.cross()
        ready_slope(1)
        update_up(1, last)
        cross_weight.back()
        low_input.back()
        if last:
            mul[1] = mu[1].astype(jnp.bfloat16)
            start(range(first, first + up_part))
            advance(8, first)
        own_act.back()
        low_grads(1, own_act.end())
        row_dot = jnp.sum(tot[1][...] * pre[1], axis=1, keepdims=True)
        coefficient = row_dot * inv[1] * inv[1] / full
        through = dot_nt(low[1], wd[1]) * d_scale
        gr[...] = gr[...] + through - coefficient * x1[...].astype(jnp.float32)
        low_act.back()
        update_up(0, last)
        update_down(1, x1t[...], last)
        weight = cross_weight.end().astype(jnp.bfloat16)
        grad_act = dot_nt(low[1], weight) - coefficient * low_input.end()
        low_grads(0, low_act.end() + grad_act)
        if last:
            return
        slope[...] = moment_decay * slope[...] + dot_nn(gram[...], low[0]) * (d_scale * d_scale)
        proj[...] = proj[...] - learn_rate * slope[...]

    def late_down(last=False):
        update_down(0, xt[...], last)

    def carried():
        first_slope.back()
        first_gram.back()
        slope[...] = first_slope.end()
        gram[...] = first_gram.end().astype(jnp.bfloat16)

    def middle(index, carry):
        def deferred():
            pl.when(index == 0)(carried)
            pl.when(index > 0)(late_down)

        step(lax.rem(index, 2), False, deferred)
        return carry

    loads[0].wait()
    xt[...] = x0_ref[...].T
    squares = row_squares(x0_ref[...])
    loads[1].wait()
    forth.begin(1, dot_nn(x0_ref[...], wd[0]) * d_scale, squares)
    loads[2].wait()
    first_slope.begin(1, dot_nn(x0_ref[...], md[0].astype(jnp.bfloat16)) * d_scale)
    first_gram.begin(1, dot_nn(x0_ref[...], xt[...]))
    forth.cross()
    first_slope.cross()
    first_gram.cross()
    for load in loads[3:]:
        load.wait()
    forth.back()
    proj[...] = forth.end()
    inv[0] = lax.rsqrt(sqs[...] / full + norm_eps)
    lax.fori_loop(0, STEPS - 1, middle, 0)
    step((STEPS - 1) % 2, True, late_down)
    if levels:
        mdl[1] = md[1].astype(jnp.bfloat16)
        mul[0] = mu[0].astype(jnp.bfloat16)
        start(range(first + up_part, len(chunks) - part))
    late_down(True)
    mdl[0] = md[0].astype(jnp.bfloat16)
    if not levels:
        mul[...] = mu[...].astype(jnp.bfloat16)
        mdl[1] = md[1].astype(jnp.bfloat16)
    outs = ((wd_out, res_wd, wd), (wu_out, res_wu, wu), (md_out, res_md, mdl), (mu_out, res_mu, mul))
    if not levels:
        stores = [pltpu.make_async_copy(kept, out, store_sem.at[k]) for k, (out, _, kept) in enumerate(outs)]
        for store in stores:
            store.start()
        for store in stores:
            store.wait()
        return
    start(range(len(chunks) - part, len(chunks)))
    advance()
    stores = []
    for piece in pieces:
        for out, res, _ in outs:
            if res is piece.res:
                stores.append(pltpu.make_async_copy(
                    piece.rows(res, 0, piece.size), piece.rows(out, 0, piece.size), store_sem.at[piece.index]
                ))
                stores[-1].start()
    for when, finish in sent:
        if when is None:
            finish()
        else:
            pl.when(when)(finish)
    for store in stores:
        store.wait()


def finish_kernel(wd_ref, wu_ref, md_ref, mu_ref, wd_out, wu_out, md_out, mu_out):
    for w_ref, m_ref, w_out, m_out in ((wd_ref, md_ref, wd_out, md_out), (wu_ref, mu_ref, wu_out, mu_out)):
        moments = m_ref[...].astype(jnp.float32)
        moved = w_ref[...].astype(jnp.float32) - learn_rate * moments
        w_out[...] = moved.astype(jnp.bfloat16)
        m_out[...] = moments


def finish(means):
    layers = means[0].shape[0]
    parts = 2
    specs = [
        pl.BlockSpec((1, mean.shape[1] // parts, mean.shape[2]), lambda i: (i // parts, i % parts, 0))
        for mean in means
    ]
    kinds = [jnp.bfloat16, jnp.bfloat16, jnp.float32, jnp.float32]
    return pl.pallas_call(
        finish_kernel,
        grid=(layers * parts,),
        out_shape=[jax.ShapeDtypeStruct(mean.shape, kind) for mean, kind in zip(means, kinds)],
        in_specs=specs,
        out_specs=specs,
    )(*means)


def fused(shards, replicas, hidden, target, w_down, w_up, m_down, m_up):
    tok, width = hidden.shape
    layers, _, rank = w_down.shape
    hops = shards // 2 - 1
    bf, f32 = jnp.bfloat16, jnp.float32
    hbm = pl.BlockSpec(memory_space=pl.ANY)
    channels = 7
    sems = channels * (2 + 2 * hops)
    rows = [tok, tok, tok, rank, tok, tok, tok]
    halves = [pltpu.VMEM((count // 2, rank), bf) for count in rows]
    crossed = [pltpu.VMEM((2 * hops, count // 2, rank), bf) for count in rows]
    totals = [pltpu.VMEM((count, rank), f32) for count in rows]
    count = 2 * layers * (len(cuts(rank, False)) + len(cuts(width, True)))
    row_sems = count * KINDS
    tripled = [(layers, 3 * count, other) for count, other in (w_down.shape[1:], w_up.shape[1:])] * 2
    return pl.pallas_call(
        functools.partial(fused_kernel, shards, replicas),
        out_shape=[
            jax.ShapeDtypeStruct(w_down.shape, bf),
            jax.ShapeDtypeStruct(w_up.shape, bf),
            jax.ShapeDtypeStruct(m_down.shape, bf),
            jax.ShapeDtypeStruct(m_up.shape, bf),
        ],
        in_specs=[hbm] * 6,
        out_specs=[hbm] * 4,
        scratch_shapes=[
            pltpu.VMEM(hidden.shape, bf),
            pltpu.VMEM(target.shape, bf),
            pltpu.VMEM(w_down.shape, bf),
            pltpu.VMEM(w_up.shape, bf),
            pltpu.VMEM(m_down.shape, f32),
            pltpu.VMEM(m_up.shape, f32),
            pltpu.SemaphoreType.DMA((6,)),
            pltpu.SemaphoreType.DMA((count,)),
            pltpu.VMEM(w_down.shape, bf),
            pltpu.VMEM(w_up.shape, bf),
            pltpu.VMEM(m_down.shape, bf),
            pltpu.VMEM(m_up.shape, bf),
            pltpu.VMEM(w_down.shape, bf),
            pltpu.VMEM(w_up.shape, bf),
            pltpu.VMEM(m_down.shape, bf),
            pltpu.VMEM(m_up.shape, bf),
            pltpu.VMEM(tripled[0], bf),
            pltpu.VMEM(tripled[1], bf),
            pltpu.VMEM(tripled[2], bf),
            pltpu.VMEM(tripled[3], bf),
            pltpu.SemaphoreType.DMA((row_sems,)),
            pltpu.SemaphoreType.DMA((row_sems,)),
            pltpu.VMEM((tok, width), bf),
            pltpu.VMEM((width, tok), bf),
            pltpu.VMEM((width, tok), bf),
            pltpu.VMEM((tok, width), f32),
            pltpu.VMEM((layers, tok, rank), f32),
            pltpu.VMEM((layers, tok, rank), f32),
            pltpu.VMEM((layers, tok, rank), bf),
            pltpu.VMEM((layers, tok, 1), f32),
            pltpu.VMEM((layers, tok, rank), bf),
            pltpu.VMEM((tok, rank), f32),
            pltpu.VMEM((tok, rank), f32),
            pltpu.VMEM((tok, tok), bf),
            pltpu.VMEM((tok, 1), f32),
            halves,
            halves,
            halves,
            crossed,
            halves,
            halves,
            totals,
            pltpu.VMEM((8, tok), f32),
            pltpu.VMEM((8, tok), f32),
            pltpu.VMEM((8, tok), f32),
            pltpu.VMEM((2 * hops, 8, tok), f32),
            pltpu.SemaphoreType.DMA((sems,)),
            pltpu.SemaphoreType.DMA((sems,)),
            pltpu.SemaphoreType.DMA((2 + 2 * hops,)),
            pltpu.SemaphoreType.DMA((2 + 2 * hops,)),
        ],
        compiler_params=pltpu.CompilerParams(
            collective_id=0, has_side_effects=True, vmem_limit_bytes=60 * 1024 * 1024
        ),
    )(hidden, target, w_down, w_up, m_down, m_up)


def body(shards, replicas, hidden, target, w_down, w_up, m_down, m_up):
    means = fused(
        shards, replicas, hidden[0], target[0], w_down[0], w_up[0], m_down[0], m_up[0]
    )
    if on_grid(replicas, hidden.shape[2], w_down.shape[3]):
        return tuple(finish(means))
    totals = lax.psum(tuple(means), "row")
    means = [total.astype(jnp.float32) / replicas for total in totals]
    return (
        means[0].astype(jnp.bfloat16),
        means[1].astype(jnp.bfloat16),
        means[2].astype(jnp.float32),
        means[3].astype(jnp.float32),
    )


def solution(mesh):
    placed = (
        P("row", None, "ta"),
        P("row", None, "ta"),
        P("row", None, "ta", None),
        P("row", None, None, "ta"),
        P("row", None, "ta", None),
        P("row", None, None, "ta"),
    )
    return jax.shard_map(
        functools.partial(body, mesh.shape["ta"], mesh.shape["row"]),
        mesh=mesh,
        in_specs=placed,
        out_specs=(
            P(None, "ta", None),
            P(None, None, "ta"),
            P(None, "ta", None),
            P(None, None, "ta"),
        ),
        check_vma=False,
    )
```

```python
import functools

import jax
import jax.numpy as jnp
from jax import lax
from jax.experimental import pallas as pl
from jax.experimental.pallas import tpu as pltpu
from jax.sharding import PartitionSpec as P

MESH = pl.DeviceIdType.MESH
STEPS = 4
norm_eps = 1e-06
learn_rate = 0.02
moment_decay = 0.9


def dot_nn(a, b):
    return jnp.dot(a, b, preferred_element_type=jnp.float32)


def dot_nt(a, b):
    return lax.dot_general(a, b, (((1,), (1,)), ((), ())), preferred_element_type=jnp.float32)


LINES = 4
LINE_SHARE = ((2, 7), (2, 7))
KINDS = 6
ORDER = [
    (0, 1), (0, 2), (2, 1), (1, 1), (5, 1), (3, 1), (4, 1), (7, 1), (0, 3), (6, 1), (1, 2), (3, 2), (2, 2),
    (2, 3), (5, 2), (4, 2), (1, 3), (3, 3), (7, 2), (8, 1), (12, 1), (1, 4), (6, 2), (0, 4), (17, 1), (5, 3),
    (10, 1), (4, 3), (9, 1), (8, 2), (6, 3), (11, 1), (13, 1), (12, 2), (3, 4), (15, 1), (10, 2), (14, 1),
    (18, 1), (16, 1), (4, 4), (0, 5), (1, 5), (7, 3), (17, 2), (2, 4), (12, 3), (9, 2), (11, 2), (8, 3),
    (4, 5), (5, 4), (17, 3), (5, 5), (6, 4), (13, 2), (9, 3), (19, 1), (11, 3), (10, 3), (8, 4), (14, 2),
    (0, 6), (13, 3), (9, 4), (12, 4), (15, 2), (3, 5), (7, 4), (10, 4), (18, 2), (16, 2), (2, 5), (4, 6),
    (17, 4), (9, 5), (13, 4), (15, 3), (6, 5), (10, 5), (19, 2), (2, 6), (11, 4), (15, 4), (18, 3), (11, 5),
    (14, 3), (7, 5), (2, 7), (5, 6), (16, 3), (1, 6), (12, 5), (18, 4), (19, 3), (7, 6), (9, 6), (3, 6),
    (14, 4), (12, 6), (17, 5), (8, 5), (15, 5), (16, 4), (17, 6), (2, 8), (18, 5), (11, 6), (19, 4), (6, 6),
    (12, 7), (14, 5), (7, 7), (17, 7), (10, 6), (13, 5), (16, 5), (19, 5), (15, 6), (7, 8), (18, 6), (13, 6),
    (8, 6), (12, 8), (16, 6), (19, 6), (14, 6), (17, 8),
]


def on_grid(replicas, width, rank):
    return replicas == 2 * LINES and width % 128 == 0 and rank % 128 == 0 and width >= 512


def cuts(length, wide, late):
    if not wide:
        return [("fold", k * (length // 2), length // 2) for k in range(2)]
    line = length * LINE_SHARE[late][0] // LINE_SHARE[late][1] // 128 * 128
    size = (length - line) // 2
    return [("line", 0, line), ("fold", line, size), ("fold", line + size, size)]


def fused_kernel(
    shards, replicas,
    x0_in, tg_in, wd_in, wu_in, md_in, mu_in,
    wd_out, wu_out, md_out, mu_out,
    x0_ref, tg_ref, wd, wu, md, mu, load_sem, store_sem, wdl, wul, mdl, mul, res_wd, res_wu, res_md, res_mu,
    got_wd, got_wu, got_md, got_mu, row_send, row_recv,
    x1, x1t, xt, gr, pre, bend, act, inv, low, proj, slope, gram, sqs, ratio,
    s1, r1, s2, r2, s3, r3, tot, q1, p1, q2, p2,
    main_send, main_recv, side_send, side_recv,
):
    tok, width = x0_ref.shape
    rank = wd.shape[2]
    loads = [
        pltpu.make_async_copy(source, target, load_sem.at[k])
        for k, (source, target) in enumerate((
            (x0_in, x0_ref), (wd_in, wd), (md_in, md), (wu_in, wu), (tg_in, tg_ref), (mu_in, mu),
        ))
    ]
    for load in loads:
        load.start()
    full = width * shards
    chips = shards // 2
    me = lax.axis_index("ta")
    core = lax.rem(me, 2)
    sibling = me + 1 - 2 * core
    partners = [lax.rem(me + 2 * k, shards) for k in range(1, chips)]
    hops = chips - 1
    d_scale = full ** (-0.5)
    r_scale = rank ** (-0.5)

    barrier = pltpu.get_barrier_semaphore()
    for peer in [sibling] + partners:
        pl.semaphore_signal(barrier, inc=1, device_id={"ta": peer}, device_id_type=MESH)
    levels = on_grid(replicas, width, rank)
    spot = lax.axis_index("row")
    line, side_of = spot // 2, lax.rem(spot, 2)
    facing = spot + 1 - 2 * side_of
    after, before = lax.rem(spot + 2, replicas), lax.rem(spot + replicas - 2, replicas)
    greeted = [facing, after, before] if levels else []
    for peer in greeted:
        pl.semaphore_signal(barrier, inc=1, device_id={"row": peer}, device_id_type=MESH)
    pl.semaphore_wait(barrier, chips + len(greeted))

    def send(src, dst, sems, index, peer):
        copy = pltpu.make_async_remote_copy(
            src_ref=src, dst_ref=dst,
            send_sem=sems[0].at[index], recv_sem=sems[1].at[index],
            device_id={"ta": peer}, device_id_type=MESH,
        )
        copy.start()
        return copy

    main = (main_send, main_recv)
    side = (side_send, side_recv)
    per_channel = 2 + 2 * hops

    def to_column(row):
        return jnp.broadcast_to(row[0:1, :], (tok, tok)).T[:, 0:1]

    def row_squares(rows):
        wide = rows.astype(jnp.float32)
        return dot_nt(jnp.ones((8, width), jnp.bfloat16), (wide * wide).astype(jnp.bfloat16))

    class Channel:
        def __init__(self, which):
            self.which = which
            self.size = tot[which].shape[0] // 2
            size = self.size
            self.mine = pl.ds(pl.multiple_of(core * size, size), size)
            self.other = pl.ds(pl.multiple_of((1 - core) * size, size), size)
            self.base = which * per_channel

        def begin(self, parity, value=None, squares=None):
            c = self.which
            self.parity = parity
            self.squares = squares is not None
            if value is not None:
                tot[c][...] = value
            s1[c][...] = tot[c][self.other, :].astype(jnp.bfloat16)
            self.copies = [send(s1[c], r1[c], main, self.base, sibling)]
            if self.squares:
                q1[...] = squares
                self.copies.append(send(q1, p1, side, 0, sibling))

        def cross(self):
            c = self.which
            for copy in self.copies:
                copy.wait()
            pair = tot[c][self.mine, :] + r1[c][...].astype(jnp.float32)
            s2[c][...] = pair.astype(jnp.bfloat16)
            spots = [self.parity * hops + k for k in range(hops)]
            self.copies = [
                send(s2[c], r2[c].at[spot], main, self.base + 2 + spot, peer)
                for spot, peer in zip(spots, partners)
            ]
            tot[c][self.mine, :] = pair
            if self.squares:
                q2[...] = q1[...] + p1[...]
                self.copies += [
                    send(q2, p2.at[spot], side, 2 + spot, peer)
                    for spot, peer in zip(spots, partners)
                ]

        def back(self):
            c = self.which
            for copy in self.copies:
                copy.wait()
            total = tot[c][self.mine, :]
            for k in range(hops):
                total = total + r2[c][self.parity * hops + k].astype(jnp.float32)
            s3[c][...] = total.astype(jnp.bfloat16)
            self.copies = [send(s3[c], r3[c], main, self.base + 1, sibling)]
            tot[c][self.mine, :] = total
            if self.squares:
                row = q2[...]
                for k in range(hops):
                    row = row + p2[self.parity * hops + k]
                sqs[...] = to_column(row)

        def end(self):
            c = self.which
            for copy in self.copies:
                copy.wait()
            tot[c][self.other, :] = r3[c][...].astype(jnp.float32)
            return tot[c][...]

    forth, own_act, low_act, cross_weight, low_input, first_slope, first_gram = [
        Channel(k) for k in range(7)
    ]

    def update(w, m, layer, grad, last):
        moment = moment_decay * m[layer] + grad
        m[layer] = moment
        if last and levels:
            return
        w[layer] = (w[layer].astype(jnp.float32) - learn_rate * moment).astype(jnp.bfloat16)

    def update_up(layer, last):
        update(wu, mu, layer, dot_nn(act[layer].T, gr[...].astype(jnp.bfloat16)) * r_scale, last)

    def update_down(layer, rows_t, last):
        update(wd, md, layer, dot_nn(rows_t, low[layer]) * d_scale, last)

    def activate(layer, preact):
        activation = (preact * jax.nn.sigmoid(preact)).astype(jnp.bfloat16)
        pre[layer] = preact
        act[layer] = activation
        return activation

    def ready_slope(layer):
        preact = pre[layer]
        sig = jax.nn.sigmoid(preact)
        steep = sig * (1.0 + preact * (1.0 - sig))
        bend[layer] = steep * inv[layer]
        pre[layer] = steep * preact

    def low_grads(layer, grad_act):
        low[layer] = (grad_act * bend[layer]).astype(jnp.bfloat16)

    down, up = (wdl, got_wd, res_wd), (wul, got_wu, res_wu)
    mdown, mup = (mdl, got_md, res_md), (mul, got_mu, res_mu)
    layers = list(reversed(range(wd.shape[0])))
    chunks = []
    for late, pairs in enumerate(((up, down), (mup, mdown))):
        for layer in layers:
            for pair, wide in zip(pairs, (False, True)):
                for form, base, size in cuts(pair[0].shape[1], wide, late):
                    chunks.append((pair, layer, form, base, size))
    first = len(chunks) // 2
    part = len(cuts(width, True, 0))
    up_part = len(cuts(rank, False, 0))
    sent = []

    class Piece:
        def __init__(self, index):
            (self.acc, self.got, self.res), self.layer, self.form, self.base, self.size = chunks[index]
            self.index = index
            self.stages = 7 if self.form == "fold" else 9

        def rows(self, ref, start, size, slot=0):
            first_row = self.base + (slot - 1 if slot else 0) * self.acc.shape[1]
            start = start + first_row
            if not isinstance(start, int):
                start = pl.multiple_of(start, 16)
            return ref.at[self.layer, pl.ds(start, size)]

        def copy(self, kind, src, dst, peer):
            index = self.index * KINDS + kind
            return pltpu.make_async_remote_copy(
                src_ref=src, dst_ref=dst,
                send_sem=row_send.at[index], recv_sem=row_recv.at[index],
                device_id={"row": peer}, device_id_type=MESH,
            )

        def sum_out(self, kind, start, size, slot, landing, peer, when=None):
            def go(finish=False):
                made = self.copy(
                    kind, self.rows(self.acc, start, size), self.rows(self.got, landing, size, slot), peer
                )
                made.wait_send() if finish else made.start()

            go()
            sent.append((when, functools.partial(go, True)))

        def mean_out(self, kind, start, size, peer, when=None):
            def go(finish=False):
                where = self.rows(self.res, start, size)
                made = self.copy(kind, where, where, peer)
                made.wait_send() if finish else made.start()

            go()
            sent.append((when, functools.partial(go, True)))

        def landed(self, kind, start, size, slot=0):
            ref = self.rows(self.got, start, size, slot) if slot else self.rows(self.res, start, size)
            self.copy(kind, ref, ref, facing).wait_recv()

        def add(self, start, size, slot, landing):
            mine = self.rows(self.acc, start, size)
            came = self.rows(self.got, landing, size, slot)
            total = mine[...].astype(jnp.float32) + came[...].astype(jnp.float32)
            mine[...] = total.astype(jnp.bfloat16)

        def settle(self, start, size, slot, landing):
            mine = self.rows(self.acc, start, size)
            came = self.rows(self.got, landing, size, slot)
            total = mine[...].astype(jnp.float32) + came[...].astype(jnp.float32)
            self.rows(self.res, start, size)[...] = (total * (1.0 / replicas)).astype(jnp.bfloat16)

        def run(self, stage):
            (self.fold if self.form == "fold" else self.line)(stage)

        def fold(self, stage):
            half_size, quarter = self.size // 2, self.size // 4
            keep, away = side_of * half_size, (1 - side_of) * half_size
            outer = (line == 0) | (line == LINES - 1)
            inner = jnp.logical_not(outer)
            upper = lax.rem(line // 2, 2)
            inward = spot + 2 - 4 * upper
            outward = spot - 2 + 4 * upper
            across = spot + 2 - 4 * upper
            own = keep + upper * quarter
            far = keep + (1 - upper) * quarter
            if stage == 0:
                self.sum_out(0, away, half_size, 1, 0, facing)
            elif stage == 1:
                self.landed(0, 0, half_size, 1)
                self.add(keep, half_size, 1, 0)

                @pl.when(outer)
                def _():
                    self.sum_out(1, keep, half_size, 2, 0, inward, outer)
            elif stage == 2:

                @pl.when(inner)
                def _():
                    self.landed(1, 0, half_size, 2)
                    self.add(keep, half_size, 2, 0)
                    self.sum_out(2, far, quarter, 3, 0, across, inner)
            elif stage == 3:

                @pl.when(inner)
                def _():
                    self.landed(2, 0, quarter, 3)
                    self.settle(own, quarter, 3, 0)
                    self.mean_out(3, own, quarter, across, inner)
            elif stage == 4:

                @pl.when(inner)
                def _():
                    self.landed(3, far, quarter)
                    self.mean_out(4, keep, half_size, outward, inner)
                    self.mean_out(5, keep, half_size, facing, inner)
            elif stage == 5:

                @pl.when(outer)
                def _():
                    self.landed(4, keep, half_size)
                    self.mean_out(5, keep, half_size, facing, outer)
            else:
                self.landed(5, away, half_size)

        def line(self, stage):
            piece = self.size // LINES
            fine = piece // 2
            end = LINES - 1
            if stage <= end:
                for at, step_to, kind, slot in ((stage, 1, 0, 1), (end - stage, -1, 1, 2)):
                    ahead = (at + 1) * piece if step_to > 0 else 0
                    count = (end - at) * piece if step_to > 0 else at * piece
                    came = (LINES - at) * piece if step_to > 0 else (at + 1) * piece
                    opened = at * piece if step_to > 0 else 0
                    here = line == at

                    @pl.when(here)
                    def _(ahead=ahead, count=count, came=came, opened=opened, kind=kind, slot=slot, here=here, peer=after if step_to > 0 else before):
                        if stage:
                            self.landed(kind, opened, came, slot)
                        if count:
                            if stage:
                                self.add(ahead, count, slot, ahead)
                            self.sum_out(kind, ahead, count, slot, ahead, peer, here)
            if stage == end:
                own = line * piece

                @pl.when(line > 0)
                def _():
                    self.add(own, piece, 1, own)

                @pl.when(line < end)
                def _():
                    self.add(own, piece, 2, own)

                self.sum_out(2, own + (1 - side_of) * fine, fine, 3, 0, facing)
            elif stage == end + 1:
                own = line * piece + side_of * fine
                self.landed(2, 0, fine, 3)
                self.settle(own, fine, 3, 0)
                self.mean_out(3, own, fine, facing)
            elif stage > end + 1:
                hop = stage - end - 2
                if hop == 0:
                    self.landed(3, line * piece + (1 - side_of) * fine, fine)
                for at, step_to, kind in ((hop, 1, 4), (end - hop, -1, 5)):
                    here = line == at
                    came = hop * piece
                    opened = 0 if step_to > 0 else (at + 1) * piece
                    begun = 0 if step_to > 0 else at * piece

                    @pl.when(here)
                    def _(came=came, opened=opened, begun=begun, kind=kind, here=here, peer=after if step_to > 0 else before):
                        if hop:
                            self.landed(kind, opened, came)
                        if hop < end:
                            self.mean_out(kind, begun, came + piece, peer, here)

    pieces = [Piece(k) for k in range(len(chunks))] if levels else []
    done = {k: 0 for k in range(len(chunks))}
    plan = list(ORDER) if levels else []

    def start(picked):
        for k in picked if levels else []:
            pieces[k].run(0)

    def advance(count=None, below=None):
        taken = 0
        for entry in list(plan):
            if taken == count:
                break
            if below is not None and entry[0] >= below:
                continue
            pieces[entry[0]].run(entry[1])
            plan.remove(entry)
            taken += 1

    def step(parity, last, deferred, nearly=False):
        activation = activate(0, proj[...] * inv[0])
        lifted = dot_nn(activation, wu[0]) * r_scale
        x1[...] = (x0_ref[...].astype(jnp.float32) + lifted).astype(jnp.bfloat16)
        forth.begin(parity, dot_nn(x1[...], wd[1]) * d_scale, row_squares(x1[...]))
        cross_weight.begin(parity, dot_nn(wu[0], wd[1]) * (r_scale * d_scale))
        forth.cross()
        low_input.begin(parity, dot_nt(x1[...], wu[0]) * r_scale)
        cross_weight.cross()
        low_input.cross()
        x1t[...] = x1[...].T
        ready_slope(0)
        deferred()
        if last:
            wdl[0] = wd[0]
            start(range(first - part, first))
            advance(5, first)
        forth.back()
        inv[1] = lax.rsqrt(sqs[...] / full + norm_eps)

        def lift(rows):
            preact = tot[0][rows, :] * inv[1, rows, :]
            activation = (preact * jax.nn.sigmoid(preact)).astype(jnp.bfloat16)
            pre[1, rows, :] = preact
            act[1, rows, :] = activation
            lifted = dot_nn(activation, wu[1]) * r_scale
            outcome = (x1[rows, :].astype(jnp.float32) + lifted).astype(jnp.bfloat16)
            gradient = outcome.astype(jnp.float32) - tg_ref[rows, :].astype(jnp.float32)
            gr[rows, :] = gradient
            tot[1][rows, :] = dot_nt(gradient.astype(jnp.bfloat16), wu[1]) * r_scale

        lift(forth.mine)
        forth.end()
        lift(forth.other)
        own_act.begin(parity)
        low_act.begin(parity, dot_nt(gr[...].astype(jnp.bfloat16), wu[0]) * r_scale)
        own_act.cross()
        low_act.cross()
        ready_slope(1)
        update_up(1, last)
        if nearly:
            wul[1] = wu[1]
            start(range(up_part))
        cross_weight.back()
        low_input.back()
        if last:
            mul[1] = mu[1].astype(jnp.bfloat16)
            start(range(first, first + up_part))
            advance(5, first)
        own_act.back()

        def lower(rows):
            grad_act = tot[1][rows, :]
            lowered = (grad_act * bend[1, rows, :]).astype(jnp.bfloat16)
            low[1, rows, :] = lowered
            row_dot = jnp.sum(grad_act * pre[1, rows, :], axis=1, keepdims=True)
            factor = row_dot * inv[1, rows, :] * inv[1, rows, :] / full
            ratio[rows, :] = factor
            through = dot_nt(lowered, wd[1]) * d_scale
            gr[rows, :] = gr[rows, :] + through - factor * x1[rows, :].astype(jnp.float32)

        lower(own_act.mine)
        own_act.end()
        lower(own_act.other)
        low_act.back()
        update_up(0, last)
        update_down(1, x1t[...], last)
        if nearly:
            wdl[1] = wd[1]
            wul[0] = wu[0]
            start(range(up_part, first - part))
            advance(1, first)
        if last:
            mdl[1] = md[1].astype(jnp.bfloat16)
            mul[0] = mu[0].astype(jnp.bfloat16)
            start(range(first + up_part, len(chunks) - part))
        weight = cross_weight.end().astype(jnp.bfloat16)
        grad_act = dot_nt(low[1], weight) - ratio[...] * low_input.end()
        low_grads(0, low_act.end() + grad_act)
        if last:
            return
        slope[...] = moment_decay * slope[...] + dot_nn(gram[...], low[0]) * (d_scale * d_scale)
        proj[...] = proj[...] - learn_rate * slope[...]

    def late_down(last=False):
        update_down(0, xt[...], last)

    def carried():
        first_slope.back()
        first_gram.back()
        slope[...] = first_slope.end()
        gram[...] = first_gram.end().astype(jnp.bfloat16)

    def middle(index, carry):
        def deferred():
            pl.when(index == 0)(carried)
            pl.when(index > 0)(late_down)

        step(lax.rem(index, 2), False, deferred)
        return carry

    loads[0].wait()
    xt[...] = x0_ref[...].T
    squares = row_squares(x0_ref[...])
    loads[1].wait()
    forth.begin(1, dot_nn(x0_ref[...], wd[0]) * d_scale, squares)
    loads[2].wait()
    first_slope.begin(1, dot_nn(x0_ref[...], md[0].astype(jnp.bfloat16)) * d_scale)
    first_gram.begin(1, dot_nn(x0_ref[...], xt[...]))
    forth.cross()
    first_slope.cross()
    first_gram.cross()
    for load in loads[3:]:
        load.wait()
    forth.back()
    proj[...] = forth.end()
    inv[0] = lax.rsqrt(sqs[...] / full + norm_eps)
    lax.fori_loop(0, STEPS - 2, middle, 0)
    step(STEPS % 2, False, late_down, nearly=bool(levels))
    step((STEPS - 1) % 2, True, late_down)
    late_down(True)
    mdl[0] = md[0].astype(jnp.bfloat16)
    if not levels:
        mul[...] = mu[...].astype(jnp.bfloat16)
        mdl[1] = md[1].astype(jnp.bfloat16)
    outs = ((wd_out, res_wd, wd), (wu_out, res_wu, wu), (md_out, res_md, mdl), (mu_out, res_mu, mul))
    if not levels:
        stores = [pltpu.make_async_copy(kept, out, store_sem.at[k]) for k, (out, _, kept) in enumerate(outs)]
        for store in stores:
            store.start()
        for store in stores:
            store.wait()
        return
    start(range(len(chunks) - part, len(chunks)))
    advance()
    stores = []
    for piece in pieces:
        for out, res, _ in outs:
            if res is piece.res:
                stores.append(pltpu.make_async_copy(
                    piece.rows(res, 0, piece.size), piece.rows(out, 0, piece.size), store_sem.at[piece.index]
                ))
                stores[-1].start()
    for when, finish in sent:
        if when is None:
            finish()
        else:
            pl.when(when)(finish)
    for store in stores:
        store.wait()


def finish_kernel(parts, *refs):
    means, outs, came, made = refs[0:4], refs[4:8], refs[8:12], refs[12:16]
    load_sem, store_sem = refs[16:]
    spots = []
    for layer in range(means[0].shape[0]):
        for part in range(parts):
            for pair in range(2):
                size = means[pair].shape[1] // parts
                spots.append((pair, layer, pl.ds(part * size, size)))

    def moved(sources, targets, sems, number, which):
        pair, layer, rows = spots[number]
        k = pair + which
        return pltpu.make_async_copy(
            sources[k].at[layer, rows], targets[k].at[layer, rows], sems.at[2 * number + which // 2]
        )

    for number in range(len(spots)):
        for which in (0, 2):
            moved(means, came, load_sem, number, which).start()
    for number, (pair, layer, rows) in enumerate(spots):
        for which in (0, 2):
            moved(means, came, load_sem, number, which).wait()
        moments = came[pair + 2][layer, rows, :].astype(jnp.float32)
        stepped = came[pair][layer, rows, :].astype(jnp.float32) - learn_rate * moments
        made[pair][layer, rows, :] = stepped.astype(jnp.bfloat16)
        made[pair + 2][layer, rows, :] = moments
        for which in (0, 2):
            moved(made, outs, store_sem, number, which).start()
    for number in range(len(spots)):
        for which in (0, 2):
            moved(made, outs, store_sem, number, which).wait()


def finish(means):
    parts = 2
    kinds = [jnp.bfloat16, jnp.bfloat16, jnp.float32, jnp.float32]
    count = 4 * parts * means[0].shape[0]
    hbm = pl.BlockSpec(memory_space=pl.ANY)
    return pl.pallas_call(
        functools.partial(finish_kernel, parts),
        out_shape=[jax.ShapeDtypeStruct(mean.shape, kind) for mean, kind in zip(means, kinds)],
        in_specs=[hbm] * 4,
        out_specs=[hbm] * 4,
        scratch_shapes=[pltpu.VMEM(mean.shape, mean.dtype) for mean in means]
        + [pltpu.VMEM(mean.shape, kind) for mean, kind in zip(means, kinds)]
        + [pltpu.SemaphoreType.DMA((count,)), pltpu.SemaphoreType.DMA((count,))],
    )(*means)


def fused(shards, replicas, hidden, target, w_down, w_up, m_down, m_up):
    tok, width = hidden.shape
    layers, _, rank = w_down.shape
    hops = shards // 2 - 1
    bf, f32 = jnp.bfloat16, jnp.float32
    hbm = pl.BlockSpec(memory_space=pl.ANY)
    channels = 7
    sems = channels * (2 + 2 * hops)
    rows = [tok, tok, tok, rank, tok, tok, tok]
    halves = [pltpu.VMEM((count // 2, rank), bf) for count in rows]
    crossed = [pltpu.VMEM((2 * hops, count // 2, rank), bf) for count in rows]
    totals = [pltpu.VMEM((count, rank), f32) for count in rows]
    count = 2 * layers * (len(cuts(rank, False, 0)) + len(cuts(width, True, 0)))
    row_sems = count * KINDS
    tripled = [(layers, 3 * count, other) for count, other in (w_down.shape[1:], w_up.shape[1:])] * 2
    return pl.pallas_call(
        functools.partial(fused_kernel, shards, replicas),
        out_shape=[
            jax.ShapeDtypeStruct(w_down.shape, bf),
            jax.ShapeDtypeStruct(w_up.shape, bf),
            jax.ShapeDtypeStruct(m_down.shape, bf),
            jax.ShapeDtypeStruct(m_up.shape, bf),
        ],
        in_specs=[hbm] * 6,
        out_specs=[hbm] * 4,
        scratch_shapes=[
            pltpu.VMEM(hidden.shape, bf),
            pltpu.VMEM(target.shape, bf),
            pltpu.VMEM(w_down.shape, bf),
            pltpu.VMEM(w_up.shape, bf),
            pltpu.VMEM(m_down.shape, f32),
            pltpu.VMEM(m_up.shape, f32),
            pltpu.SemaphoreType.DMA((6,)),
            pltpu.SemaphoreType.DMA((count,)),
            pltpu.VMEM(w_down.shape, bf),
            pltpu.VMEM(w_up.shape, bf),
            pltpu.VMEM(m_down.shape, bf),
            pltpu.VMEM(m_up.shape, bf),
            pltpu.VMEM(w_down.shape, bf),
            pltpu.VMEM(w_up.shape, bf),
            pltpu.VMEM(m_down.shape, bf),
            pltpu.VMEM(m_up.shape, bf),
            pltpu.VMEM(tripled[0], bf),
            pltpu.VMEM(tripled[1], bf),
            pltpu.VMEM(tripled[2], bf),
            pltpu.VMEM(tripled[3], bf),
            pltpu.SemaphoreType.DMA((row_sems,)),
            pltpu.SemaphoreType.DMA((row_sems,)),
            pltpu.VMEM((tok, width), bf),
            pltpu.VMEM((width, tok), bf),
            pltpu.VMEM((width, tok), bf),
            pltpu.VMEM((tok, width), f32),
            pltpu.VMEM((layers, tok, rank), f32),
            pltpu.VMEM((layers, tok, rank), f32),
            pltpu.VMEM((layers, tok, rank), bf),
            pltpu.VMEM((layers, tok, 1), f32),
            pltpu.VMEM((layers, tok, rank), bf),
            pltpu.VMEM((tok, rank), f32),
            pltpu.VMEM((tok, rank), f32),
            pltpu.VMEM((tok, tok), bf),
            pltpu.VMEM((tok, 1), f32),
            pltpu.VMEM((tok, 1), f32),
            halves,
            halves,
            halves,
            crossed,
            halves,
            halves,
            totals,
            pltpu.VMEM((8, tok), f32),
            pltpu.VMEM((8, tok), f32),
            pltpu.VMEM((8, tok), f32),
            pltpu.VMEM((2 * hops, 8, tok), f32),
            pltpu.SemaphoreType.DMA((sems,)),
            pltpu.SemaphoreType.DMA((sems,)),
            pltpu.SemaphoreType.DMA((2 + 2 * hops,)),
            pltpu.SemaphoreType.DMA((2 + 2 * hops,)),
        ],
        compiler_params=pltpu.CompilerParams(
            collective_id=0, has_side_effects=True, vmem_limit_bytes=60 * 1024 * 1024
        ),
    )(hidden, target, w_down, w_up, m_down, m_up)


def body(shards, replicas, hidden, target, w_down, w_up, m_down, m_up):
    means = fused(
        shards, replicas, hidden[0], target[0], w_down[0], w_up[0], m_down[0], m_up[0]
    )
    if on_grid(replicas, hidden.shape[2], w_down.shape[3]):
        return tuple(finish(means))
    totals = lax.psum(tuple(means), "row")
    means = [total.astype(jnp.float32) / replicas for total in totals]
    return (
        means[0].astype(jnp.bfloat16),
        means[1].astype(jnp.bfloat16),
        means[2].astype(jnp.float32),
        means[3].astype(jnp.float32),
    )


def solution(mesh):
    placed = (
        P("row", None, "ta"),
        P("row", None, "ta"),
        P("row", None, "ta", None),
        P("row", None, None, "ta"),
        P("row", None, "ta", None),
        P("row", None, None, "ta"),
    )
    return jax.shard_map(
        functools.partial(body, mesh.shape["ta"], mesh.shape["row"]),
        mesh=mesh,
        in_specs=placed,
        out_specs=(
            P(None, "ta", None),
            P(None, None, "ta"),
            P(None, "ta", None),
            P(None, None, "ta"),
        ),
        check_vma=False,
    )
```

```python
import functools

import jax
import jax.numpy as jnp
from jax import lax
from jax.experimental import pallas as pl
from jax.experimental.pallas import tpu as pltpu
from jax.sharding import PartitionSpec as P

MESH = pl.DeviceIdType.MESH
STEPS = 4
norm_eps = 1e-06
learn_rate = 0.02
moment_decay = 0.9


def dot_nn(a, b):
    return jnp.dot(a, b, preferred_element_type=jnp.float32)


def dot_nt(a, b):
    return lax.dot_general(a, b, (((1,), (1,)), ((), ())), preferred_element_type=jnp.float32)


LINES = 4
LINE_SHARE = ((2, 7), (2, 7))
KINDS = 6
ORDER = [
    (0, 1), (0, 2), (2, 1), (1, 1), (5, 1), (3, 1), (4, 1), (7, 1), (0, 3), (6, 1), (1, 2), (3, 2), (2, 2),
    (2, 3), (5, 2), (4, 2), (1, 3), (3, 3), (7, 2), (8, 1), (12, 1), (1, 4), (6, 2), (0, 4), (17, 1), (5, 3),
    (10, 1), (4, 3), (9, 1), (8, 2), (6, 3), (11, 1), (13, 1), (12, 2), (3, 4), (15, 1), (10, 2), (14, 1),
    (18, 1), (16, 1), (4, 4), (0, 5), (1, 5), (7, 3), (17, 2), (2, 4), (12, 3), (9, 2), (11, 2), (8, 3),
    (4, 5), (5, 4), (17, 3), (5, 5), (6, 4), (13, 2), (9, 3), (19, 1), (11, 3), (10, 3), (8, 4), (14, 2),
    (0, 6), (13, 3), (9, 4), (12, 4), (15, 2), (3, 5), (7, 4), (10, 4), (18, 2), (16, 2), (2, 5), (4, 6),
    (17, 4), (9, 5), (13, 4), (15, 3), (6, 5), (10, 5), (19, 2), (2, 6), (11, 4), (15, 4), (18, 3), (11, 5),
    (14, 3), (7, 5), (2, 7), (5, 6), (16, 3), (1, 6), (12, 5), (18, 4), (19, 3), (7, 6), (9, 6), (3, 6),
    (14, 4), (12, 6), (17, 5), (8, 5), (15, 5), (16, 4), (17, 6), (2, 8), (18, 5), (11, 6), (19, 4), (6, 6),
    (12, 7), (14, 5), (7, 7), (17, 7), (10, 6), (13, 5), (16, 5), (19, 5), (15, 6), (7, 8), (18, 6), (13, 6),
    (8, 6), (12, 8), (16, 6), (19, 6), (14, 6), (17, 8),
]


def on_grid(replicas, width, rank):
    return replicas == 2 * LINES and width % 128 == 0 and rank % 128 == 0 and width >= 512


def cuts(length, wide, late):
    if not wide:
        return [("fold", k * (length // 2), length // 2) for k in range(2)]
    line = length * LINE_SHARE[late][0] // LINE_SHARE[late][1] // 128 * 128
    size = (length - line) // 2
    return [("line", 0, line), ("fold", line, size), ("fold", line + size, size)]


def fused_kernel(
    shards, replicas,
    x0_in, tg_in, wd_in, wu_in, md_in, mu_in,
    wd_out, wu_out, md_out, mu_out,
    x0_ref, tg_ref, wd, wu, md, mu, load_sem, store_sem, wdl, wul, mdl, mul, res_wd, res_wu, res_md, res_mu,
    got_wd, got_wu, got_md, got_mu, row_send, row_recv,
    x1, x1t, xt, gr, pre, bend, act, inv, low, proj, slope, gram, sqs, ratio,
    s1, r1, s2, r2, s3, r3, tot, q1, p1, q2, p2,
    main_send, main_recv, side_send, side_recv,
):
    tok, width = x0_ref.shape
    rank = wd.shape[2]
    loads = [
        pltpu.make_async_copy(source, target, load_sem.at[k])
        for k, (source, target) in enumerate((
            (x0_in, x0_ref), (wd_in, wd), (md_in, md), (wu_in, wu), (tg_in, tg_ref), (mu_in, mu),
        ))
    ]
    for load in loads:
        load.start()
    full = width * shards
    chips = shards // 2
    me = lax.axis_index("ta")
    core = lax.rem(me, 2)
    sibling = me + 1 - 2 * core
    partners = [lax.rem(me + 2 * k, shards) for k in range(1, chips)]
    hops = chips - 1
    d_scale = full ** (-0.5)
    r_scale = rank ** (-0.5)

    barrier = pltpu.get_barrier_semaphore()
    for peer in [sibling] + partners:
        pl.semaphore_signal(barrier, inc=1, device_id={"ta": peer}, device_id_type=MESH)
    levels = on_grid(replicas, width, rank)
    spot = lax.axis_index("row")
    line, side_of = spot // 2, lax.rem(spot, 2)
    facing = spot + 1 - 2 * side_of
    after, before = lax.rem(spot + 2, replicas), lax.rem(spot + replicas - 2, replicas)
    at_end = (line == 0) | (line == LINES - 1)

    def greet(peer):
        pl.semaphore_signal(barrier, inc=1, device_id={"row": peer}, device_id_type=MESH)

    if levels:
        greet(facing)
        pl.when(line < LINES - 1)(lambda: greet(after))
        pl.when(line > 0)(lambda: greet(before))

    def send(src, dst, sems, index, peer):
        copy = pltpu.make_async_remote_copy(
            src_ref=src, dst_ref=dst,
            send_sem=sems[0].at[index], recv_sem=sems[1].at[index],
            device_id={"ta": peer}, device_id_type=MESH,
        )
        copy.start()
        return copy

    main = (main_send, main_recv)
    side = (side_send, side_recv)
    per_channel = 2 + 2 * hops

    def to_column(row):
        return jnp.broadcast_to(row[0:1, :], (tok, tok)).T[:, 0:1]

    def row_squares(rows):
        wide = rows.astype(jnp.float32)
        return dot_nt(jnp.ones((8, width), jnp.bfloat16), (wide * wide).astype(jnp.bfloat16))

    class Channel:
        def __init__(self, which):
            self.which = which
            self.size = tot[which].shape[0] // 2
            size = self.size
            self.mine = pl.ds(pl.multiple_of(core * size, size), size)
            self.other = pl.ds(pl.multiple_of((1 - core) * size, size), size)
            self.base = which * per_channel

        def begin(self, parity, value=None, squares=None):
            c = self.which
            self.parity = parity
            self.squares = squares is not None
            if value is not None:
                tot[c][...] = value
            s1[c][...] = tot[c][self.other, :].astype(jnp.bfloat16)
            self.copies = [send(s1[c], r1[c], main, self.base, sibling)]
            if self.squares:
                q1[...] = squares
                self.copies.append(send(q1, p1, side, 0, sibling))

        def cross(self):
            c = self.which
            for copy in self.copies:
                copy.wait()
            pair = tot[c][self.mine, :] + r1[c][...].astype(jnp.float32)
            s2[c][...] = pair.astype(jnp.bfloat16)
            spots = [self.parity * hops + k for k in range(hops)]
            self.copies = [
                send(s2[c], r2[c].at[spot], main, self.base + 2 + spot, peer)
                for spot, peer in zip(spots, partners)
            ]
            tot[c][self.mine, :] = pair
            if self.squares:
                q2[...] = q1[...] + p1[...]
                self.copies += [
                    send(q2, p2.at[spot], side, 2 + spot, peer)
                    for spot, peer in zip(spots, partners)
                ]

        def back(self):
            c = self.which
            for copy in self.copies:
                copy.wait()
            total = tot[c][self.mine, :]
            for k in range(hops):
                total = total + r2[c][self.parity * hops + k].astype(jnp.float32)
            s3[c][...] = total.astype(jnp.bfloat16)
            self.copies = [send(s3[c], r3[c], main, self.base + 1, sibling)]
            tot[c][self.mine, :] = total
            if self.squares:
                row = q2[...]
                for k in range(hops):
                    row = row + p2[self.parity * hops + k]
                sqs[...] = to_column(row)

        def end(self):
            c = self.which
            for copy in self.copies:
                copy.wait()
            tot[c][self.other, :] = r3[c][...].astype(jnp.float32)
            return tot[c][...]

    forth, own_act, low_act, cross_weight, low_input, first_slope, first_gram = [
        Channel(k) for k in range(7)
    ]

    def update(w, m, layer, grad, last):
        moment = moment_decay * m[layer] + grad
        m[layer] = moment
        if last and levels:
            return
        w[layer] = (w[layer].astype(jnp.float32) - learn_rate * moment).astype(jnp.bfloat16)

    def update_up(layer, last):
        update(wu, mu, layer, dot_nn(act[layer].T, gr[...].astype(jnp.bfloat16)) * r_scale, last)

    def update_down(layer, rows_t, last):
        update(wd, md, layer, dot_nn(rows_t, low[layer]) * d_scale, last)

    def activate(layer, preact):
        activation = (preact * jax.nn.sigmoid(preact)).astype(jnp.bfloat16)
        pre[layer] = preact
        act[layer] = activation
        return activation

    def ready_slope(layer):
        preact = pre[layer]
        sig = jax.nn.sigmoid(preact)
        steep = sig * (1.0 + preact * (1.0 - sig))
        bend[layer] = steep * inv[layer]
        pre[layer] = steep * preact

    def low_grads(layer, grad_act):
        low[layer] = (grad_act * bend[layer]).astype(jnp.bfloat16)

    down, up = (wdl, got_wd, res_wd), (wul, got_wu, res_wu)
    mdown, mup = (mdl, got_md, res_md), (mul, got_mu, res_mu)
    layers = list(reversed(range(wd.shape[0])))
    chunks = []
    for late, pairs in enumerate(((up, down), (mup, mdown))):
        for layer in layers:
            for pair, wide in zip(pairs, (False, True)):
                for form, base, size in cuts(pair[0].shape[1], wide, late):
                    chunks.append((pair, layer, form, base, size))
    first = len(chunks) // 2
    part = len(cuts(width, True, 0))
    up_part = len(cuts(rank, False, 0))
    sent = []

    class Piece:
        def __init__(self, index):
            (self.acc, self.got, self.res), self.layer, self.form, self.base, self.size = chunks[index]
            self.index = index
            self.stages = 7 if self.form == "fold" else 9

        def rows(self, ref, start, size, slot=0):
            first_row = self.base + (slot - 1 if slot else 0) * self.acc.shape[1]
            start = start + first_row
            if not isinstance(start, int):
                start = pl.multiple_of(start, 16)
            return ref.at[self.layer, pl.ds(start, size)]

        def copy(self, kind, src, dst, peer):
            index = self.index * KINDS + kind
            return pltpu.make_async_remote_copy(
                src_ref=src, dst_ref=dst,
                send_sem=row_send.at[index], recv_sem=row_recv.at[index],
                device_id={"row": peer}, device_id_type=MESH,
            )

        def sum_out(self, kind, start, size, slot, landing, peer, when=None):
            def go(finish=False):
                made = self.copy(
                    kind, self.rows(self.acc, start, size), self.rows(self.got, landing, size, slot), peer
                )
                made.wait_send() if finish else made.start()

            go()
            sent.append((when, functools.partial(go, True)))

        def mean_out(self, kind, start, size, peer, when=None):
            def go(finish=False):
                where = self.rows(self.res, start, size)
                made = self.copy(kind, where, where, peer)
                made.wait_send() if finish else made.start()

            go()
            sent.append((when, functools.partial(go, True)))

        def landed(self, kind, start, size, slot=0):
            ref = self.rows(self.got, start, size, slot) if slot else self.rows(self.res, start, size)
            self.copy(kind, ref, ref, facing).wait_recv()

        def add(self, start, size, slot, landing):
            mine = self.rows(self.acc, start, size)
            came = self.rows(self.got, landing, size, slot)
            total = mine[...].astype(jnp.float32) + came[...].astype(jnp.float32)
            mine[...] = total.astype(jnp.bfloat16)

        def settle(self, start, size, slot, landing):
            mine = self.rows(self.acc, start, size)
            came = self.rows(self.got, landing, size, slot)
            total = mine[...].astype(jnp.float32) + came[...].astype(jnp.float32)
            self.rows(self.res, start, size)[...] = (total * (1.0 / replicas)).astype(jnp.bfloat16)

        def run(self, stage):
            (self.fold if self.form == "fold" else self.line)(stage)

        def fold(self, stage):
            half_size, quarter = self.size // 2, self.size // 4
            keep, away = side_of * half_size, (1 - side_of) * half_size
            outer = (line == 0) | (line == LINES - 1)
            inner = jnp.logical_not(outer)
            upper = lax.rem(line // 2, 2)
            inward = spot + 2 - 4 * upper
            outward = spot - 2 + 4 * upper
            across = spot + 2 - 4 * upper
            own = keep + upper * quarter
            far = keep + (1 - upper) * quarter
            if stage == 0:
                self.sum_out(0, away, half_size, 1, 0, facing)
            elif stage == 1:
                self.landed(0, 0, half_size, 1)
                self.add(keep, half_size, 1, 0)

                @pl.when(outer)
                def _():
                    self.sum_out(1, keep, half_size, 2, 0, inward, outer)
            elif stage == 2:

                @pl.when(inner)
                def _():
                    self.landed(1, 0, half_size, 2)
                    self.add(keep, half_size, 2, 0)
                    self.sum_out(2, far, quarter, 3, 0, across, inner)
            elif stage == 3:

                @pl.when(inner)
                def _():
                    self.landed(2, 0, quarter, 3)
                    self.settle(own, quarter, 3, 0)
                    self.mean_out(3, own, quarter, across, inner)
            elif stage == 4:

                @pl.when(inner)
                def _():
                    self.landed(3, far, quarter)
                    self.mean_out(4, keep, half_size, outward, inner)
                    self.mean_out(5, keep, half_size, facing, inner)
            elif stage == 5:

                @pl.when(outer)
                def _():
                    self.landed(4, keep, half_size)
                    self.mean_out(5, keep, half_size, facing, outer)
            else:
                self.landed(5, away, half_size)

        def line(self, stage):
            piece = self.size // LINES
            fine = piece // 2
            end = LINES - 1
            if stage <= end:
                for at, step_to, kind, slot in ((stage, 1, 0, 1), (end - stage, -1, 1, 2)):
                    ahead = (at + 1) * piece if step_to > 0 else 0
                    count = (end - at) * piece if step_to > 0 else at * piece
                    came = (LINES - at) * piece if step_to > 0 else (at + 1) * piece
                    opened = at * piece if step_to > 0 else 0
                    here = line == at

                    @pl.when(here)
                    def _(ahead=ahead, count=count, came=came, opened=opened, kind=kind, slot=slot, here=here, peer=after if step_to > 0 else before):
                        if stage:
                            self.landed(kind, opened, came, slot)
                        if count:
                            if stage:
                                self.add(ahead, count, slot, ahead)
                            self.sum_out(kind, ahead, count, slot, ahead, peer, here)
            if stage == end:
                own = line * piece

                @pl.when(line > 0)
                def _():
                    self.add(own, piece, 1, own)

                @pl.when(line < end)
                def _():
                    self.add(own, piece, 2, own)

                self.sum_out(2, own + (1 - side_of) * fine, fine, 3, 0, facing)
            elif stage == end + 1:
                own = line * piece + side_of * fine
                self.landed(2, 0, fine, 3)
                self.settle(own, fine, 3, 0)
                self.mean_out(3, own, fine, facing)
            elif stage > end + 1:
                hop = stage - end - 2
                if hop == 0:
                    self.landed(3, line * piece + (1 - side_of) * fine, fine)
                for at, step_to, kind in ((hop, 1, 4), (end - hop, -1, 5)):
                    here = line == at
                    came = hop * piece
                    opened = 0 if step_to > 0 else (at + 1) * piece
                    begun = 0 if step_to > 0 else at * piece

                    @pl.when(here)
                    def _(came=came, opened=opened, begun=begun, kind=kind, here=here, peer=after if step_to > 0 else before):
                        if hop:
                            self.landed(kind, opened, came)
                        if hop < end:
                            self.mean_out(kind, begun, came + piece, peer, here)

    pieces = [Piece(k) for k in range(len(chunks))] if levels else []
    done = {k: 0 for k in range(len(chunks))}
    plan = list(ORDER) if levels else []

    def start(picked):
        for k in picked if levels else []:
            pieces[k].run(0)

    outs = ((wd_out, res_wd, wd), (wu_out, res_wu, wu), (md_out, res_md, mdl), (mu_out, res_mu, mul))
    stowed = []

    def stow(piece):
        for out, res, _ in outs:
            if res is piece.res:
                stowed.append(pltpu.make_async_copy(
                    piece.rows(res, 0, piece.size), piece.rows(out, 0, piece.size), store_sem.at[piece.index]
                ))
                stowed[-1].start()

    def advance(count=None, below=None):
        taken = 0
        for entry in list(plan):
            if taken == count:
                break
            if below is not None and entry[0] >= below:
                continue
            piece = pieces[entry[0]]
            piece.run(entry[1])
            if entry[1] == piece.stages - 1:
                stow(piece)
            plan.remove(entry)
            taken += 1

    def step(parity, last, deferred, nearly=False):
        activation = activate(0, proj[...] * inv[0])
        lifted = dot_nn(activation, wu[0]) * r_scale
        x1[...] = (x0_ref[...].astype(jnp.float32) + lifted).astype(jnp.bfloat16)
        forth.begin(parity, dot_nn(x1[...], wd[1]) * d_scale, row_squares(x1[...]))
        cross_weight.begin(parity, dot_nn(wu[0], wd[1]) * (r_scale * d_scale))
        forth.cross()
        low_input.begin(parity, dot_nt(x1[...], wu[0]) * r_scale)
        cross_weight.cross()
        low_input.cross()
        x1t[...] = x1[...].T
        ready_slope(0)
        deferred()
        if last:
            wdl[0] = wd[0]
            start(range(first - part, first))
            advance(5, first)
        forth.back()
        inv[1] = lax.rsqrt(sqs[...] / full + norm_eps)

        def lift(rows):
            preact = tot[0][rows, :] * inv[1, rows, :]
            activation = (preact * jax.nn.sigmoid(preact)).astype(jnp.bfloat16)
            pre[1, rows, :] = preact
            act[1, rows, :] = activation
            lifted = dot_nn(activation, wu[1]) * r_scale
            outcome = (x1[rows, :].astype(jnp.float32) + lifted).astype(jnp.bfloat16)
            gradient = outcome.astype(jnp.float32) - tg_ref[rows, :].astype(jnp.float32)
            gr[rows, :] = gradient
            tot[1][rows, :] = dot_nt(gradient.astype(jnp.bfloat16), wu[1]) * r_scale

        lift(forth.mine)
        forth.end()
        lift(forth.other)
        own_act.begin(parity)
        low_act.begin(parity, dot_nt(gr[...].astype(jnp.bfloat16), wu[0]) * r_scale)
        own_act.cross()
        low_act.cross()
        ready_slope(1)
        update_up(1, last)
        if nearly:
            wul[1] = wu[1]
            start(range(up_part))
        cross_weight.back()
        low_input.back()
        if last:
            mul[1] = mu[1].astype(jnp.bfloat16)
            start(range(first, first + up_part))
            advance(5, first)
        own_act.back()

        def lower(rows):
            grad_act = tot[1][rows, :]
            lowered = (grad_act * bend[1, rows, :]).astype(jnp.bfloat16)
            low[1, rows, :] = lowered
            row_dot = jnp.sum(grad_act * pre[1, rows, :], axis=1, keepdims=True)
            factor = row_dot * inv[1, rows, :] * inv[1, rows, :] / full
            ratio[rows, :] = factor
            through = dot_nt(lowered, wd[1]) * d_scale
            gr[rows, :] = gr[rows, :] + through - factor * x1[rows, :].astype(jnp.float32)

        lower(own_act.mine)
        own_act.end()
        lower(own_act.other)
        low_act.back()
        update_up(0, last)
        update_down(1, x1t[...], last)
        if nearly:
            wdl[1] = wd[1]
            wul[0] = wu[0]
            start(range(up_part, first - part))
            advance(1, first)
        if last:
            mdl[1] = md[1].astype(jnp.bfloat16)
            mul[0] = mu[0].astype(jnp.bfloat16)
            start(range(first + up_part, len(chunks) - part))
        weight = cross_weight.end().astype(jnp.bfloat16)
        grad_act = dot_nt(low[1], weight) - ratio[...] * low_input.end()
        low_grads(0, low_act.end() + grad_act)
        if last:
            return
        slope[...] = moment_decay * slope[...] + dot_nn(gram[...], low[0]) * (d_scale * d_scale)
        proj[...] = proj[...] - learn_rate * slope[...]

    def late_down(last=False):
        update_down(0, xt[...], last)

    def carried():
        first_slope.back()
        first_gram.back()
        slope[...] = first_slope.end()
        gram[...] = first_gram.end().astype(jnp.bfloat16)

    def middle(index, carry):
        def deferred():
            pl.when(index == 0)(carried)
            pl.when(index > 0)(late_down)

        step(lax.rem(index, 2), False, deferred)
        return carry

    loads[0].wait()
    xt[...] = x0_ref[...].T
    q1[...] = row_squares(x0_ref[...])
    loads[1].wait()
    tot[0][...] = dot_nn(x0_ref[...], wd[0]) * d_scale
    pl.semaphore_wait(barrier, chips + (jnp.where(at_end, 2, 3) if levels else 0))
    forth.begin(1, squares=q1[...])
    loads[2].wait()
    first_slope.begin(1, dot_nn(x0_ref[...], md[0].astype(jnp.bfloat16)) * d_scale)
    first_gram.begin(1, dot_nn(x0_ref[...], xt[...]))
    forth.cross()
    first_slope.cross()
    first_gram.cross()
    for load in loads[3:]:
        load.wait()
    forth.back()
    proj[...] = forth.end()
    inv[0] = lax.rsqrt(sqs[...] / full + norm_eps)
    lax.fori_loop(0, STEPS - 2, middle, 0)
    step(STEPS % 2, False, late_down, nearly=bool(levels))
    step((STEPS - 1) % 2, True, late_down)
    late_down(True)
    mdl[0] = md[0].astype(jnp.bfloat16)
    if not levels:
        mul[...] = mu[...].astype(jnp.bfloat16)
        mdl[1] = md[1].astype(jnp.bfloat16)
    if not levels:
        stores = [pltpu.make_async_copy(kept, out, store_sem.at[k]) for k, (out, _, kept) in enumerate(outs)]
        for store in stores:
            store.start()
        for store in stores:
            store.wait()
        return
    start(range(len(chunks) - part, len(chunks)))
    advance()
    for when, finish in sent:
        if when is None:
            finish()
        else:
            pl.when(when)(finish)
    for store in stowed:
        store.wait()


def finish_kernel(parts, *refs):
    means, outs, came, made = refs[0:4], refs[4:8], refs[8:12], refs[12:16]
    load_sem, store_sem = refs[16:]
    spots = []
    for layer in range(means[0].shape[0]):
        for part in range(parts):
            for pair in range(2):
                size = means[pair].shape[1] // parts
                spots.append((pair, layer, pl.ds(part * size, size)))

    def moved(sources, targets, sems, number, which):
        pair, layer, rows = spots[number]
        k = pair + which
        return pltpu.make_async_copy(
            sources[k].at[layer, rows], targets[k].at[layer, rows], sems.at[2 * number + which // 2]
        )

    for number in range(len(spots)):
        for which in (0, 2):
            moved(means, came, load_sem, number, which).start()
    for number, (pair, layer, rows) in enumerate(spots):
        for which in (0, 2):
            moved(means, came, load_sem, number, which).wait()
        moments = came[pair + 2][layer, rows, :].astype(jnp.float32)
        stepped = came[pair][layer, rows, :].astype(jnp.float32) - learn_rate * moments
        made[pair][layer, rows, :] = stepped.astype(jnp.bfloat16)
        made[pair + 2][layer, rows, :] = moments
        for which in (0, 2):
            moved(made, outs, store_sem, number, which).start()
    for number in range(len(spots)):
        for which in (0, 2):
            moved(made, outs, store_sem, number, which).wait()


def finish(means):
    parts = 2
    kinds = [jnp.bfloat16, jnp.bfloat16, jnp.float32, jnp.float32]
    count = 4 * parts * means[0].shape[0]
    hbm = pl.BlockSpec(memory_space=pl.ANY)
    return pl.pallas_call(
        functools.partial(finish_kernel, parts),
        out_shape=[jax.ShapeDtypeStruct(mean.shape, kind) for mean, kind in zip(means, kinds)],
        in_specs=[hbm] * 4,
        out_specs=[hbm] * 4,
        scratch_shapes=[pltpu.VMEM(mean.shape, mean.dtype) for mean in means]
        + [pltpu.VMEM(mean.shape, kind) for mean, kind in zip(means, kinds)]
        + [pltpu.SemaphoreType.DMA((count,)), pltpu.SemaphoreType.DMA((count,))],
    )(*means)


def fused(shards, replicas, hidden, target, w_down, w_up, m_down, m_up):
    tok, width = hidden.shape
    layers, _, rank = w_down.shape
    hops = shards // 2 - 1
    bf, f32 = jnp.bfloat16, jnp.float32
    hbm = pl.BlockSpec(memory_space=pl.ANY)
    channels = 7
    sems = channels * (2 + 2 * hops)
    rows = [tok, tok, tok, rank, tok, tok, tok]
    halves = [pltpu.VMEM((count // 2, rank), bf) for count in rows]
    crossed = [pltpu.VMEM((2 * hops, count // 2, rank), bf) for count in rows]
    totals = [pltpu.VMEM((count, rank), f32) for count in rows]
    count = 2 * layers * (len(cuts(rank, False, 0)) + len(cuts(width, True, 0)))
    row_sems = count * KINDS
    tripled = [(layers, 3 * count, other) for count, other in (w_down.shape[1:], w_up.shape[1:])] * 2
    return pl.pallas_call(
        functools.partial(fused_kernel, shards, replicas),
        out_shape=[
            jax.ShapeDtypeStruct(w_down.shape, bf),
            jax.ShapeDtypeStruct(w_up.shape, bf),
            jax.ShapeDtypeStruct(m_down.shape, bf),
            jax.ShapeDtypeStruct(m_up.shape, bf),
        ],
        in_specs=[hbm] * 6,
        out_specs=[hbm] * 4,
        scratch_shapes=[
            pltpu.VMEM(hidden.shape, bf),
            pltpu.VMEM(target.shape, bf),
            pltpu.VMEM(w_down.shape, bf),
            pltpu.VMEM(w_up.shape, bf),
            pltpu.VMEM(m_down.shape, f32),
            pltpu.VMEM(m_up.shape, f32),
            pltpu.SemaphoreType.DMA((6,)),
            pltpu.SemaphoreType.DMA((count,)),
            pltpu.VMEM(w_down.shape, bf),
            pltpu.VMEM(w_up.shape, bf),
            pltpu.VMEM(m_down.shape, bf),
            pltpu.VMEM(m_up.shape, bf),
            pltpu.VMEM(w_down.shape, bf),
            pltpu.VMEM(w_up.shape, bf),
            pltpu.VMEM(m_down.shape, bf),
            pltpu.VMEM(m_up.shape, bf),
            pltpu.VMEM(tripled[0], bf),
            pltpu.VMEM(tripled[1], bf),
            pltpu.VMEM(tripled[2], bf),
            pltpu.VMEM(tripled[3], bf),
            pltpu.SemaphoreType.DMA((row_sems,)),
            pltpu.SemaphoreType.DMA((row_sems,)),
            pltpu.VMEM((tok, width), bf),
            pltpu.VMEM((width, tok), bf),
            pltpu.VMEM((width, tok), bf),
            pltpu.VMEM((tok, width), f32),
            pltpu.VMEM((layers, tok, rank), f32),
            pltpu.VMEM((layers, tok, rank), f32),
            pltpu.VMEM((layers, tok, rank), bf),
            pltpu.VMEM((layers, tok, 1), f32),
            pltpu.VMEM((layers, tok, rank), bf),
            pltpu.VMEM((tok, rank), f32),
            pltpu.VMEM((tok, rank), f32),
            pltpu.VMEM((tok, tok), bf),
            pltpu.VMEM((tok, 1), f32),
            pltpu.VMEM((tok, 1), f32),
            halves,
            halves,
            halves,
            crossed,
            halves,
            halves,
            totals,
            pltpu.VMEM((8, tok), f32),
            pltpu.VMEM((8, tok), f32),
            pltpu.VMEM((8, tok), f32),
            pltpu.VMEM((2 * hops, 8, tok), f32),
            pltpu.SemaphoreType.DMA((sems,)),
            pltpu.SemaphoreType.DMA((sems,)),
            pltpu.SemaphoreType.DMA((2 + 2 * hops,)),
            pltpu.SemaphoreType.DMA((2 + 2 * hops,)),
        ],
        compiler_params=pltpu.CompilerParams(
            collective_id=0, has_side_effects=True, vmem_limit_bytes=60 * 1024 * 1024
        ),
    )(hidden, target, w_down, w_up, m_down, m_up)


def body(shards, replicas, hidden, target, w_down, w_up, m_down, m_up):
    means = fused(
        shards, replicas, hidden[0], target[0], w_down[0], w_up[0], m_down[0], m_up[0]
    )
    if on_grid(replicas, hidden.shape[2], w_down.shape[3]):
        return tuple(finish(means))
    totals = lax.psum(tuple(means), "row")
    means = [total.astype(jnp.float32) / replicas for total in totals]
    return (
        means[0].astype(jnp.bfloat16),
        means[1].astype(jnp.bfloat16),
        means[2].astype(jnp.float32),
        means[3].astype(jnp.float32),
    )


def solution(mesh):
    placed = (
        P("row", None, "ta"),
        P("row", None, "ta"),
        P("row", None, "ta", None),
        P("row", None, None, "ta"),
        P("row", None, "ta", None),
        P("row", None, None, "ta"),
    )
    return jax.shard_map(
        functools.partial(body, mesh.shape["ta"], mesh.shape["row"]),
        mesh=mesh,
        in_specs=placed,
        out_specs=(
            P(None, "ta", None),
            P(None, None, "ta"),
            P(None, "ta", None),
            P(None, None, "ta"),
        ),
        check_vma=False,
    )
```

```python
import functools

import jax
import jax.numpy as jnp
from jax import lax
from jax.experimental import pallas as pl
from jax.experimental.pallas import tpu as pltpu
from jax.sharding import PartitionSpec as P

MESH = pl.DeviceIdType.MESH
STEPS = 4
norm_eps = 1e-06
learn_rate = 0.02
moment_decay = 0.9


def dot_nn(a, b):
    return jnp.dot(a, b, preferred_element_type=jnp.float32)


def dot_nt(a, b):
    return lax.dot_general(a, b, (((1,), (1,)), ((), ())), preferred_element_type=jnp.float32)


LINES = 4
LINE_SHARE = ((2, 7), (2, 7))
KINDS = 6
ORDER = [
    (0, 1), (0, 2), (2, 1), (1, 1), (5, 1), (3, 1), (4, 1), (7, 1), (0, 3), (6, 1), (1, 2), (3, 2), (2, 2),
    (2, 3), (5, 2), (4, 2), (1, 3), (3, 3), (7, 2), (8, 1), (12, 1), (1, 4), (6, 2), (0, 4), (17, 1), (5, 3),
    (10, 1), (4, 3), (9, 1), (8, 2), (6, 3), (11, 1), (13, 1), (12, 2), (3, 4), (15, 1), (10, 2), (14, 1),
    (18, 1), (16, 1), (4, 4), (0, 5), (1, 5), (7, 3), (17, 2), (2, 4), (12, 3), (9, 2), (11, 2), (8, 3),
    (4, 5), (5, 4), (17, 3), (5, 5), (6, 4), (13, 2), (9, 3), (19, 1), (11, 3), (10, 3), (8, 4), (14, 2),
    (0, 6), (13, 3), (9, 4), (12, 4), (15, 2), (3, 5), (7, 4), (10, 4), (18, 2), (16, 2), (2, 5), (4, 6),
    (17, 4), (9, 5), (13, 4), (15, 3), (6, 5), (10, 5), (19, 2), (2, 6), (11, 4), (15, 4), (18, 3), (11, 5),
    (14, 3), (7, 5), (2, 7), (5, 6), (16, 3), (1, 6), (12, 5), (18, 4), (19, 3), (7, 6), (9, 6), (3, 6),
    (14, 4), (12, 6), (17, 5), (8, 5), (15, 5), (16, 4), (17, 6), (2, 8), (18, 5), (11, 6), (19, 4), (6, 6),
    (12, 7), (14, 5), (7, 7), (17, 7), (10, 6), (13, 5), (16, 5), (19, 5), (15, 6), (7, 8), (18, 6), (13, 6),
    (8, 6), (12, 8), (16, 6), (19, 6), (14, 6), (17, 8),
]


def on_grid(replicas, width, rank):
    return replicas == 2 * LINES and width % 128 == 0 and rank % 128 == 0 and width >= 512


def cuts(length, wide, late):
    if not wide:
        return [("fold", k * (length // 2), length // 2) for k in range(2)]
    line = length * LINE_SHARE[late][0] // LINE_SHARE[late][1] // 128 * 128
    size = (length - line) // 2
    return [("line", 0, line), ("fold", line, size), ("fold", line + size, size)]


def fused_kernel(
    shards, replicas,
    x0_in, tg_in, wd_in, wu_in, md_in, mu_in,
    wd_out, wu_out, md_out, mu_out,
    x0_ref, tg_ref, wd, wu, md, mu, load_sem, store_sem, wdl, wul, mdl, mul, res_wd, res_wu, res_md, res_mu,
    got_wd, got_wu, got_md, got_mu, row_send, row_recv,
    x1, x1t, xt, gr, pre, bend, act, inv, low, proj, slope, gram, sqs, ratio,
    s1, r1, s2, r2, s3, r3, tot, q1, p1, q2, p2,
    main_send, main_recv, side_send, side_recv,
):
    tok, width = x0_ref.shape
    rank = wd.shape[2]
    loads = [
        pltpu.make_async_copy(source, target, load_sem.at[k])
        for k, (source, target) in enumerate((
            (x0_in, x0_ref), (wd_in, wd), (md_in, md), (wu_in, wu), (tg_in, tg_ref), (mu_in, mu),
        ))
    ]
    for load in loads:
        load.start()
    full = width * shards
    chips = shards // 2
    me = lax.axis_index("ta")
    core = lax.rem(me, 2)
    sibling = me + 1 - 2 * core
    partners = [lax.rem(me + 2 * k, shards) for k in range(1, chips)]
    hops = chips - 1
    d_scale = full ** (-0.5)
    r_scale = rank ** (-0.5)

    barrier = pltpu.get_barrier_semaphore()
    for peer in [sibling] + partners:
        pl.semaphore_signal(barrier, inc=1, device_id={"ta": peer}, device_id_type=MESH)
    levels = on_grid(replicas, width, rank)
    spot = lax.axis_index("row")
    line, side_of = spot // 2, lax.rem(spot, 2)
    facing = spot + 1 - 2 * side_of
    after, before = lax.rem(spot + 2, replicas), lax.rem(spot + replicas - 2, replicas)
    at_end = (line == 0) | (line == LINES - 1)

    def greet(peer):
        pl.semaphore_signal(barrier, inc=1, device_id={"row": peer}, device_id_type=MESH)

    if levels:
        greet(facing)
        pl.when(line < LINES - 1)(lambda: greet(after))
        pl.when(line > 0)(lambda: greet(before))

    def send(src, dst, sems, index, peer):
        copy = pltpu.make_async_remote_copy(
            src_ref=src, dst_ref=dst,
            send_sem=sems[0].at[index], recv_sem=sems[1].at[index],
            device_id={"ta": peer}, device_id_type=MESH,
        )
        copy.start()
        return copy

    main = (main_send, main_recv)
    side = (side_send, side_recv)
    per_channel = 2 + 2 * hops

    def to_column(row):
        return jnp.broadcast_to(row[0:1, :], (tok, tok)).T[:, 0:1]

    def row_squares(rows):
        wide = rows.astype(jnp.float32)
        return dot_nt(jnp.ones((8, width), jnp.bfloat16), (wide * wide).astype(jnp.bfloat16))

    class Channel:
        def __init__(self, which):
            self.which = which
            self.size = tot[which].shape[0] // 2
            size = self.size
            self.mine = pl.ds(pl.multiple_of(core * size, size), size)
            self.other = pl.ds(pl.multiple_of((1 - core) * size, size), size)
            self.base = which * per_channel

        def begin(self, parity, value=None, squares=None):
            c = self.which
            self.parity = parity
            self.squares = squares is not None
            if value is not None:
                tot[c][...] = value
            s1[c][...] = tot[c][self.other, :].astype(jnp.bfloat16)
            self.copies = [send(s1[c], r1[c], main, self.base, sibling)]
            if self.squares:
                q1[...] = squares
                self.copies.append(send(q1, p1, side, 0, sibling))

        def cross(self):
            c = self.which
            for copy in self.copies:
                copy.wait()
            pair = tot[c][self.mine, :] + r1[c][...].astype(jnp.float32)
            s2[c][...] = pair.astype(jnp.bfloat16)
            spots = [self.parity * hops + k for k in range(hops)]
            self.copies = [
                send(s2[c], r2[c].at[spot], main, self.base + 2 + spot, peer)
                for spot, peer in zip(spots, partners)
            ]
            tot[c][self.mine, :] = pair
            if self.squares:
                q2[...] = q1[...] + p1[...]
                self.copies += [
                    send(q2, p2.at[spot], side, 2 + spot, peer)
                    for spot, peer in zip(spots, partners)
                ]

        def back(self):
            c = self.which
            for copy in self.copies:
                copy.wait()
            total = tot[c][self.mine, :]
            for k in range(hops):
                total = total + r2[c][self.parity * hops + k].astype(jnp.float32)
            s3[c][...] = total.astype(jnp.bfloat16)
            self.copies = [send(s3[c], r3[c], main, self.base + 1, sibling)]
            tot[c][self.mine, :] = total
            if self.squares:
                row = q2[...]
                for k in range(hops):
                    row = row + p2[self.parity * hops + k]
                sqs[...] = to_column(row)

        def end(self):
            c = self.which
            for copy in self.copies:
                copy.wait()
            tot[c][self.other, :] = r3[c][...].astype(jnp.float32)
            return tot[c][...]

    forth, own_act, low_act, cross_weight, low_input, first_slope, first_gram = [
        Channel(k) for k in range(7)
    ]

    def update(w, m, layer, grad, last):
        moment = moment_decay * m[layer] + grad
        m[layer] = moment
        if last and levels:
            return
        w[layer] = (w[layer].astype(jnp.float32) - learn_rate * moment).astype(jnp.bfloat16)

    def update_up(layer, last):
        update(wu, mu, layer, dot_nn(act[layer].T, gr[...].astype(jnp.bfloat16)) * r_scale, last)

    def update_down(layer, rows_t, last):
        update(wd, md, layer, dot_nn(rows_t, low[layer]) * d_scale, last)

    def activate(layer, preact):
        activation = (preact * jax.nn.sigmoid(preact)).astype(jnp.bfloat16)
        pre[layer] = preact
        act[layer] = activation
        return activation

    def ready_slope(layer):
        preact = pre[layer]
        sig = jax.nn.sigmoid(preact)
        steep = sig * (1.0 + preact * (1.0 - sig))
        bend[layer] = steep * inv[layer]
        pre[layer] = steep * preact

    def low_grads(layer, grad_act):
        low[layer] = (grad_act * bend[layer]).astype(jnp.bfloat16)

    down, up = (wdl, got_wd, res_wd), (wul, got_wu, res_wu)
    mdown, mup = (mdl, got_md, res_md), (mul, got_mu, res_mu)
    layers = list(reversed(range(wd.shape[0])))
    chunks = []
    for late, pairs in enumerate(((up, down), (mup, mdown))):
        for layer in layers:
            for pair, wide in zip(pairs, (False, True)):
                for form, base, size in cuts(pair[0].shape[1], wide, late):
                    chunks.append((pair, layer, form, base, size))
    first = len(chunks) // 2
    part = len(cuts(width, True, 0))
    up_part = len(cuts(rank, False, 0))
    sent = []

    class Piece:
        def __init__(self, index):
            (self.acc, self.got, self.res), self.layer, self.form, self.base, self.size = chunks[index]
            self.index = index
            self.stages = 7 if self.form == "fold" else 9

        def rows(self, ref, start, size, slot=0):
            first_row = self.base + (slot - 1 if slot else 0) * self.acc.shape[1]
            start = start + first_row
            if not isinstance(start, int):
                start = pl.multiple_of(start, 16)
            return ref.at[self.layer, pl.ds(start, size)]

        def copy(self, kind, src, dst, peer):
            index = self.index * KINDS + kind
            return pltpu.make_async_remote_copy(
                src_ref=src, dst_ref=dst,
                send_sem=row_send.at[index], recv_sem=row_recv.at[index],
                device_id={"row": peer}, device_id_type=MESH,
            )

        def sum_out(self, kind, start, size, slot, landing, peer, when=None):
            def go(finish=False):
                made = self.copy(
                    kind, self.rows(self.acc, start, size), self.rows(self.got, landing, size, slot), peer
                )
                made.wait_send() if finish else made.start()

            go()
            sent.append((when, functools.partial(go, True)))

        def mean_out(self, kind, start, size, peer, when=None):
            def go(finish=False):
                where = self.rows(self.res, start, size)
                made = self.copy(kind, where, where, peer)
                made.wait_send() if finish else made.start()

            go()
            sent.append((when, functools.partial(go, True)))

        def landed(self, kind, start, size, slot=0):
            ref = self.rows(self.got, start, size, slot) if slot else self.rows(self.res, start, size)
            self.copy(kind, ref, ref, facing).wait_recv()

        def add(self, start, size, slot, landing):
            mine = self.rows(self.acc, start, size)
            came = self.rows(self.got, landing, size, slot)
            total = mine[...].astype(jnp.float32) + came[...].astype(jnp.float32)
            mine[...] = total.astype(jnp.bfloat16)

        def settle(self, start, size, slot, landing):
            mine = self.rows(self.acc, start, size)
            came = self.rows(self.got, landing, size, slot)
            total = mine[...].astype(jnp.float32) + came[...].astype(jnp.float32)
            self.rows(self.res, start, size)[...] = (total * (1.0 / replicas)).astype(jnp.bfloat16)

        def run(self, stage):
            (self.fold if self.form == "fold" else self.line)(stage)

        def fold(self, stage):
            half_size, quarter = self.size // 2, self.size // 4
            keep, away = side_of * half_size, (1 - side_of) * half_size
            outer = (line == 0) | (line == LINES - 1)
            inner = jnp.logical_not(outer)
            upper = lax.rem(line // 2, 2)
            inward = spot + 2 - 4 * upper
            outward = spot - 2 + 4 * upper
            across = spot + 2 - 4 * upper
            own = keep + upper * quarter
            far = keep + (1 - upper) * quarter
            if stage == 0:
                self.sum_out(0, away, half_size, 1, 0, facing)
            elif stage == 1:
                self.landed(0, 0, half_size, 1)
                self.add(keep, half_size, 1, 0)

                @pl.when(outer)
                def _():
                    self.sum_out(1, keep, half_size, 2, 0, inward, outer)
            elif stage == 2:

                @pl.when(inner)
                def _():
                    self.landed(1, 0, half_size, 2)
                    self.add(keep, half_size, 2, 0)
                    self.sum_out(2, far, quarter, 3, 0, across, inner)
            elif stage == 3:

                @pl.when(inner)
                def _():
                    self.landed(2, 0, quarter, 3)
                    self.settle(own, quarter, 3, 0)
                    self.mean_out(3, own, quarter, across, inner)
            elif stage == 4:

                @pl.when(inner)
                def _():
                    self.landed(3, far, quarter)
                    self.mean_out(4, keep, half_size, outward, inner)
                    self.mean_out(5, keep, half_size, facing, inner)
            elif stage == 5:

                @pl.when(outer)
                def _():
                    self.landed(4, keep, half_size)
                    self.mean_out(5, keep, half_size, facing, outer)
            else:
                self.landed(5, away, half_size)

        def line(self, stage):
            piece = self.size // LINES
            fine = piece // 2
            end = LINES - 1
            if stage <= end:
                for at, step_to, kind, slot in ((stage, 1, 0, 1), (end - stage, -1, 1, 2)):
                    ahead = (at + 1) * piece if step_to > 0 else 0
                    count = (end - at) * piece if step_to > 0 else at * piece
                    came = (LINES - at) * piece if step_to > 0 else (at + 1) * piece
                    opened = at * piece if step_to > 0 else 0
                    here = line == at

                    @pl.when(here)
                    def _(ahead=ahead, count=count, came=came, opened=opened, kind=kind, slot=slot, here=here, peer=after if step_to > 0 else before):
                        if stage:
                            self.landed(kind, opened, came, slot)
                        if count:
                            if stage:
                                self.add(ahead, count, slot, ahead)
                            self.sum_out(kind, ahead, count, slot, ahead, peer, here)
            if stage == end:
                own = line * piece

                @pl.when(line > 0)
                def _():
                    self.add(own, piece, 1, own)

                @pl.when(line < end)
                def _():
                    self.add(own, piece, 2, own)

                self.sum_out(2, own + (1 - side_of) * fine, fine, 3, 0, facing)
            elif stage == end + 1:
                own = line * piece + side_of * fine
                self.landed(2, 0, fine, 3)
                self.settle(own, fine, 3, 0)
                self.mean_out(3, own, fine, facing)
            elif stage > end + 1:
                hop = stage - end - 2
                if hop == 0:
                    self.landed(3, line * piece + (1 - side_of) * fine, fine)
                for at, step_to, kind in ((hop, 1, 4), (end - hop, -1, 5)):
                    here = line == at
                    came = hop * piece
                    opened = 0 if step_to > 0 else (at + 1) * piece
                    begun = 0 if step_to > 0 else at * piece

                    @pl.when(here)
                    def _(came=came, opened=opened, begun=begun, kind=kind, here=here, peer=after if step_to > 0 else before):
                        if hop:
                            self.landed(kind, opened, came)
                        if hop < end:
                            self.mean_out(kind, begun, came + piece, peer, here)

    pieces = [Piece(k) for k in range(len(chunks))] if levels else []
    done = {k: 0 for k in range(len(chunks))}
    plan = list(ORDER) if levels else []

    def start(picked):
        for k in picked if levels else []:
            pieces[k].run(0)

    outs = ((wd_out, res_wd, wd), (wu_out, res_wu, wu), (md_out, res_md, mdl), (mu_out, res_mu, mul))
    stowed = []

    def stow(piece):
        for out, res, _ in outs:
            if res is piece.res:
                stowed.append(pltpu.make_async_copy(
                    piece.rows(res, 0, piece.size), piece.rows(out, 0, piece.size), store_sem.at[piece.index]
                ))
                stowed[-1].start()

    def advance(count=None, below=None):
        taken = 0
        for entry in list(plan):
            if taken == count:
                break
            if below is not None and entry[0] >= below:
                continue
            piece = pieces[entry[0]]
            piece.run(entry[1])
            if entry[1] == piece.stages - 1:
                stow(piece)
            plan.remove(entry)
            taken += 1

    def step(parity, last, deferred, nearly=False):
        activation = activate(0, proj[...] * inv[0])
        lifted = dot_nn(activation, wu[0]) * r_scale
        x1[...] = (x0_ref[...].astype(jnp.float32) + lifted).astype(jnp.bfloat16)
        forth.begin(parity, dot_nn(x1[...], wd[1]) * d_scale, row_squares(x1[...]))
        cross_weight.begin(parity, dot_nn(wu[0], wd[1]) * (r_scale * d_scale))
        forth.cross()
        low_input.begin(parity, dot_nt(x1[...], wu[0]) * r_scale)
        cross_weight.cross()
        low_input.cross()
        x1t[...] = x1[...].T
        ready_slope(0)
        deferred()
        if last:
            wdl[0] = wd[0]
            start(range(first - part, first))
            advance(5, first)
        forth.back()
        inv[1] = lax.rsqrt(sqs[...] / full + norm_eps)

        def lift(rows):
            preact = tot[0][rows, :] * inv[1, rows, :]
            activation = (preact * jax.nn.sigmoid(preact)).astype(jnp.bfloat16)
            pre[1, rows, :] = preact
            act[1, rows, :] = activation
            lifted = dot_nn(activation, wu[1]) * r_scale
            outcome = (x1[rows, :].astype(jnp.float32) + lifted).astype(jnp.bfloat16)
            gradient = outcome.astype(jnp.float32) - tg_ref[rows, :].astype(jnp.float32)
            gr[rows, :] = gradient
            tot[1][rows, :] = dot_nt(gradient.astype(jnp.bfloat16), wu[1]) * r_scale

        lift(forth.mine)
        forth.end()
        lift(forth.other)
        own_act.begin(parity)
        low_act.begin(parity, dot_nt(gr[...].astype(jnp.bfloat16), wu[0]) * r_scale)
        own_act.cross()
        low_act.cross()
        ready_slope(1)
        update_up(1, last)
        if nearly:
            wul[1] = wu[1]
            start(range(up_part))
        cross_weight.back()
        low_input.back()
        if last:
            mul[1] = mu[1].astype(jnp.bfloat16)
            start(range(first, first + up_part))
            advance(5, first)
        own_act.back()

        def lower(rows):
            grad_act = tot[1][rows, :]
            lowered = (grad_act * bend[1, rows, :]).astype(jnp.bfloat16)
            low[1, rows, :] = lowered
            row_dot = jnp.sum(grad_act * pre[1, rows, :], axis=1, keepdims=True)
            factor = row_dot * inv[1, rows, :] * inv[1, rows, :] / full
            ratio[rows, :] = factor
            through = dot_nt(lowered, wd[1]) * d_scale
            gr[rows, :] = gr[rows, :] + through - factor * x1[rows, :].astype(jnp.float32)

        lower(own_act.mine)
        own_act.end()
        lower(own_act.other)
        low_act.back()
        update_up(0, last)
        update_down(1, x1t[...], last)
        if nearly:
            wdl[1] = wd[1]
            wul[0] = wu[0]
            start(range(up_part, first - part))
            advance(1, first)
        if last:
            mdl[1] = md[1].astype(jnp.bfloat16)
            mul[0] = mu[0].astype(jnp.bfloat16)
            start(range(first + up_part, len(chunks) - part))
        weight = cross_weight.end().astype(jnp.bfloat16)
        grad_act = dot_nt(low[1], weight) - ratio[...] * low_input.end()
        low_grads(0, low_act.end() + grad_act)
        if last:
            return
        slope[...] = moment_decay * slope[...] + dot_nn(gram[...], low[0]) * (d_scale * d_scale)
        proj[...] = proj[...] - learn_rate * slope[...]

    def late_down(last=False):
        update_down(0, xt[...], last)

    def carried():
        first_slope.back()
        first_gram.back()
        slope[...] = first_slope.end()
        gram[...] = first_gram.end().astype(jnp.bfloat16)

    def middle(index, carry):
        def deferred():
            pl.when(index == 0)(carried)
            pl.when(index > 0)(late_down)

        step(lax.rem(index, 2), False, deferred)
        return carry

    loads[0].wait()
    xt[...] = x0_ref[...].T
    q1[...] = row_squares(x0_ref[...])
    loads[1].wait()
    tot[0][...] = dot_nn(x0_ref[...], wd[0]) * d_scale
    pl.semaphore_wait(barrier, chips + (jnp.where(at_end, 2, 3) if levels else 0))
    forth.begin(1, squares=q1[...])
    loads[2].wait()
    first_slope.begin(1, dot_nn(x0_ref[...], md[0].astype(jnp.bfloat16)) * d_scale)
    first_gram.begin(1, dot_nn(x0_ref[...], xt[...]))
    forth.cross()
    first_slope.cross()
    first_gram.cross()
    for load in loads[3:]:
        load.wait()
    forth.back()
    proj[...] = forth.end()
    inv[0] = lax.rsqrt(sqs[...] / full + norm_eps)
    lax.fori_loop(0, STEPS - 2, middle, 0)
    step(STEPS % 2, False, late_down, nearly=bool(levels))
    step((STEPS - 1) % 2, True, late_down)
    late_down(True)
    mdl[0] = md[0].astype(jnp.bfloat16)
    if not levels:
        mul[...] = mu[...].astype(jnp.bfloat16)
        mdl[1] = md[1].astype(jnp.bfloat16)
    if not levels:
        stores = [pltpu.make_async_copy(kept, out, store_sem.at[k]) for k, (out, _, kept) in enumerate(outs)]
        for store in stores:
            store.start()
        for store in stores:
            store.wait()
        return
    start(range(len(chunks) - part, len(chunks)))
    advance()
    for when, finish in sent:
        if when is None:
            finish()
        else:
            pl.when(when)(finish)
    for store in stowed:
        store.wait()


def finish_kernel(parts, *refs):
    means, outs, came, made = refs[0:4], refs[4:8], refs[8:12], refs[12:16]
    load_sem, store_sem = refs[16:]
    spots = []
    for layer in range(means[0].shape[0]):
        for part in range(parts):
            for pair in range(2):
                size = means[pair].shape[1] // parts
                spots.append((pair, layer, pl.ds(part * size, size)))

    def moved(sources, targets, sems, number, which):
        pair, layer, rows = spots[number]
        k = pair + which
        return pltpu.make_async_copy(
            sources[k].at[layer, rows], targets[k].at[layer, rows], sems.at[2 * number + which // 2]
        )

    for number in range(len(spots)):
        for which in (0, 2):
            moved(means, came, load_sem, number, which).start()
    for number, (pair, layer, rows) in enumerate(spots):
        for which in (0, 2):
            moved(means, came, load_sem, number, which).wait()
        moments = came[pair + 2][layer, rows, :].astype(jnp.float32)
        stepped = came[pair][layer, rows, :].astype(jnp.float32) - learn_rate * moments
        made[pair][layer, rows, :] = stepped.astype(jnp.bfloat16)
        made[pair + 2][layer, rows, :] = moments
        for which in (0, 2):
            moved(made, outs, store_sem, number, which).start()
    for number in range(len(spots)):
        for which in (0, 2):
            moved(made, outs, store_sem, number, which).wait()


def finish(means):
    parts = 4
    kinds = [jnp.bfloat16, jnp.bfloat16, jnp.float32, jnp.float32]
    count = 4 * parts * means[0].shape[0]
    hbm = pl.BlockSpec(memory_space=pl.ANY)
    return pl.pallas_call(
        functools.partial(finish_kernel, parts),
        out_shape=[jax.ShapeDtypeStruct(mean.shape, kind) for mean, kind in zip(means, kinds)],
        in_specs=[hbm] * 4,
        out_specs=[hbm] * 4,
        scratch_shapes=[pltpu.VMEM(mean.shape, mean.dtype) for mean in means]
        + [pltpu.VMEM(mean.shape, kind) for mean, kind in zip(means, kinds)]
        + [pltpu.SemaphoreType.DMA((count,)), pltpu.SemaphoreType.DMA((count,))],
    )(*means)


def fused(shards, replicas, hidden, target, w_down, w_up, m_down, m_up):
    tok, width = hidden.shape
    layers, _, rank = w_down.shape
    hops = shards // 2 - 1
    bf, f32 = jnp.bfloat16, jnp.float32
    hbm = pl.BlockSpec(memory_space=pl.ANY)
    channels = 7
    sems = channels * (2 + 2 * hops)
    rows = [tok, tok, tok, rank, tok, tok, tok]
    halves = [pltpu.VMEM((count // 2, rank), bf) for count in rows]
    crossed = [pltpu.VMEM((2 * hops, count // 2, rank), bf) for count in rows]
    totals = [pltpu.VMEM((count, rank), f32) for count in rows]
    count = 2 * layers * (len(cuts(rank, False, 0)) + len(cuts(width, True, 0)))
    row_sems = count * KINDS
    tripled = [(layers, 3 * count, other) for count, other in (w_down.shape[1:], w_up.shape[1:])] * 2
    return pl.pallas_call(
        functools.partial(fused_kernel, shards, replicas),
        out_shape=[
            jax.ShapeDtypeStruct(w_down.shape, bf),
            jax.ShapeDtypeStruct(w_up.shape, bf),
            jax.ShapeDtypeStruct(m_down.shape, bf),
            jax.ShapeDtypeStruct(m_up.shape, bf),
        ],
        in_specs=[hbm] * 6,
        out_specs=[hbm] * 4,
        scratch_shapes=[
            pltpu.VMEM(hidden.shape, bf),
            pltpu.VMEM(target.shape, bf),
            pltpu.VMEM(w_down.shape, bf),
            pltpu.VMEM(w_up.shape, bf),
            pltpu.VMEM(m_down.shape, f32),
            pltpu.VMEM(m_up.shape, f32),
            pltpu.SemaphoreType.DMA((6,)),
            pltpu.SemaphoreType.DMA((count,)),
            pltpu.VMEM(w_down.shape, bf),
            pltpu.VMEM(w_up.shape, bf),
            pltpu.VMEM(m_down.shape, bf),
            pltpu.VMEM(m_up.shape, bf),
            pltpu.VMEM(w_down.shape, bf),
            pltpu.VMEM(w_up.shape, bf),
            pltpu.VMEM(m_down.shape, bf),
            pltpu.VMEM(m_up.shape, bf),
            pltpu.VMEM(tripled[0], bf),
            pltpu.VMEM(tripled[1], bf),
            pltpu.VMEM(tripled[2], bf),
            pltpu.VMEM(tripled[3], bf),
            pltpu.SemaphoreType.DMA((row_sems,)),
            pltpu.SemaphoreType.DMA((row_sems,)),
            pltpu.VMEM((tok, width), bf),
            pltpu.VMEM((width, tok), bf),
            pltpu.VMEM((width, tok), bf),
            pltpu.VMEM((tok, width), f32),
            pltpu.VMEM((layers, tok, rank), f32),
            pltpu.VMEM((layers, tok, rank), f32),
            pltpu.VMEM((layers, tok, rank), bf),
            pltpu.VMEM((layers, tok, 1), f32),
            pltpu.VMEM((layers, tok, rank), bf),
            pltpu.VMEM((tok, rank), f32),
            pltpu.VMEM((tok, rank), f32),
            pltpu.VMEM((tok, tok), bf),
            pltpu.VMEM((tok, 1), f32),
            pltpu.VMEM((tok, 1), f32),
            halves,
            halves,
            halves,
            crossed,
            halves,
            halves,
            totals,
            pltpu.VMEM((8, tok), f32),
            pltpu.VMEM((8, tok), f32),
            pltpu.VMEM((8, tok), f32),
            pltpu.VMEM((2 * hops, 8, tok), f32),
            pltpu.SemaphoreType.DMA((sems,)),
            pltpu.SemaphoreType.DMA((sems,)),
            pltpu.SemaphoreType.DMA((2 + 2 * hops,)),
            pltpu.SemaphoreType.DMA((2 + 2 * hops,)),
        ],
        compiler_params=pltpu.CompilerParams(
            collective_id=0, has_side_effects=True, vmem_limit_bytes=60 * 1024 * 1024
        ),
    )(hidden, target, w_down, w_up, m_down, m_up)


def body(shards, replicas, hidden, target, w_down, w_up, m_down, m_up):
    means = fused(
        shards, replicas, hidden[0], target[0], w_down[0], w_up[0], m_down[0], m_up[0]
    )
    if on_grid(replicas, hidden.shape[2], w_down.shape[3]):
        return tuple(finish(means))
    totals = lax.psum(tuple(means), "row")
    means = [total.astype(jnp.float32) / replicas for total in totals]
    return (
        means[0].astype(jnp.bfloat16),
        means[1].astype(jnp.bfloat16),
        means[2].astype(jnp.float32),
        means[3].astype(jnp.float32),
    )


def solution(mesh):
    placed = (
        P("row", None, "ta"),
        P("row", None, "ta"),
        P("row", None, "ta", None),
        P("row", None, None, "ta"),
        P("row", None, "ta", None),
        P("row", None, None, "ta"),
    )
    return jax.shard_map(
        functools.partial(body, mesh.shape["ta"], mesh.shape["row"]),
        mesh=mesh,
        in_specs=placed,
        out_specs=(
            P(None, "ta", None),
            P(None, None, "ta"),
            P(None, "ta", None),
            P(None, None, "ta"),
        ),
        check_vma=False,
    )
```
